128 devices in a mesh: dp: 8 (over x, z_lo), tensor: 16 (over y, z_hi, core).
Axes of the slice: x: 4, y: 4, z: 4 (z_hi: 2, z_lo: 2; z = z_hi * 2 + z_lo), core: 2. Of those that a mesh axis runs over, the one named last changes fastest.
Arguments:
- hidden_act: bfloat16 [5632, 36864], P('dp', 'tensor'), may hold values from -80 to 80
- out_grad: bfloat16 [5632, 4608], P('dp', 'tensor'), may hold values from -0.5 to 0.5
- other_sq: float32 [16], P('dp'), may hold values from 2989699 to 597939968
Outputs:
- weight_grad: float32 [4608, 36864], P('dp', 'tensor')
The draws below stay inside these ranges and needn't reach their ends.
All inputs are finite; a program needn't handle non-finite values.
Results may differ from the reference program's by a relative error of at most 0.002.
Values may be sent and summed in bfloat16 or wider, within the bound.
A program may use at most 128 MiB of HBM per device.

```python
import math
import jax
import jax.numpy as jnp
from jax import lax

D = 4608
FF = 36864
L = 352
EX_DEV = 2
EXAMPLES = 16
TOKENS = 5632
N_DP = 8


def draw_hidden_act(key, part):
    base_key = jax.random.fold_in(key, 11)
    noise_key = jax.random.fold_in(base_key, 0)
    column_key = jax.random.fold_in(base_key, 1)
    share_key = jax.random.fold_in(base_key, 3)
    factor_key = jax.random.fold_in(base_key, 4)
    values = jax.random.truncated_normal(noise_key, -3.0, 3.0, (EXAMPLES, L, FF), jnp.float32)
    ramp = 3.0 ** (jnp.arange(FF, dtype=jnp.float32) / FF)
    column_scale = ramp * jax.random.uniform(column_key, (FF,), jnp.float32, 0.5, 1.5)
    share_ratio = 0.85 / math.sqrt(L)
    direction = jax.random.truncated_normal(share_key, -3.0, 3.0, (EXAMPLES, 1, FF), jnp.float32) * math.sqrt(share_ratio)
    factor = jnp.exp(jax.random.uniform(factor_key, (EXAMPLES, L, 1), jnp.float32, math.log(0.5), math.log(2.0)))
    values = (values + factor * direction) * column_scale[None, None, :]
    values = values.reshape(TOKENS, FF)
    return jnp.clip(values, -80.0, 80.0).astype(jnp.bfloat16)


def draw_out_grad(key, part):
    base_key = jax.random.fold_in(key, 23)
    noise_key, share_key, factor_key, pair_key = jax.random.split(base_key, 4)
    sigma = 0.02
    share_ratio = 0.85 / math.sqrt(L)
    noise = jax.random.truncated_normal(noise_key, -4.0, 4.0, (EXAMPLES, L, D), jnp.float32) * sigma
    direction = jax.random.truncated_normal(share_key, -3.0, 3.0, (EXAMPLES, 1, D), jnp.float32) * (sigma * math.sqrt(share_ratio))
    factor = jnp.exp(jax.random.uniform(factor_key, (EXAMPLES, L, 1), jnp.float32, math.log(0.5), math.log(2.0)))
    values = (noise + factor * direction).reshape(TOKENS, D)
    groups = EXAMPLES // EX_DEV
    target = jax.random.permutation(pair_key, groups)
    row_group = jnp.arange(TOKENS, dtype=jnp.int32) // (EX_DEV * L)
    column_group = jnp.arange(D, dtype=jnp.int32) // (D // groups)
    paired = target[row_group][:, None] == column_group[None, :]
    values = values * jnp.where(paired, 3.0, 1.0)
    return jnp.clip(values, -0.5, 0.5).astype(jnp.bfloat16)


def steps_of(stream_key, dims, pieces, low, largest):
    def one(dim, shards_of):
        heights = jax.random.uniform(jax.random.fold_in(jax.random.fold_in(stream_key, 6), dim), (shards_of,), jnp.float32, low / len(pieces), largest / len(pieces))
        return jnp.repeat(jnp.exp(heights), dims[dim] // shards_of).reshape((-1,) + (1,) * (len(dims) - dim - 1))

    level = one(*pieces[0])
    for cut in pieces[1:]:
        level = level * one(*cut)
    return level


def setup_inputs(seed: int = 0) -> dict:
    key_list = jax.random.split(jax.random.key(seed), 4)
    return {
        "hidden_act": draw_hidden_act(jax.random.fold_in(key_list[3], 71), 0),
        "out_grad": draw_out_grad(jax.random.fold_in(key_list[3], 71), 0),
        "other_sq": jnp.clip(jnp.exp(math.log(597939968) - 5.2983176 * jax.random.uniform(key_list[2], (EXAMPLES,), jnp.float32) ** steps_of(key_list[2], (EXAMPLES,), ((0, 8),), -0.2, 0.2)), 2989699, 597939968),
    }


def reference(hidden_act, out_grad, other_sq):
    acts = hidden_act.astype(jnp.float32).reshape(EXAMPLES, L, FF)
    grads = out_grad.astype(jnp.float32).reshape(EXAMPLES, L, D)
    act_gram = jnp.einsum('etf,esf->ets', acts, acts, precision=lax.Precision.HIGHEST)
    grad_gram = jnp.einsum('etd,esd->ets', grads, grads, precision=lax.Precision.HIGHEST)
    layer_sq = lax.optimization_barrier(jnp.sum(act_gram * grad_gram, axis=(1, 2)))
    clip_bound = math.sqrt(L * FF * D / 80.0)
    clip_scale = jnp.minimum(1.0, clip_bound / jnp.sqrt(other_sq + layer_sq))
    scaled_grad = (grads * clip_scale[:, None, None]).astype(jnp.bfloat16).reshape(TOKENS, D)
    group_rows = EX_DEV * L
    running = jnp.zeros((D, FF), jnp.float32)
    for group in range(N_DP):
        columns = scaled_grad[group * group_rows:(group + 1) * group_rows].astype(jnp.float32)
        activations = hidden_act[group * group_rows:(group + 1) * group_rows].astype(jnp.float32)
        running = running + jnp.dot(columns.T, activations, precision=lax.Precision.HIGHEST)
    return running
```

```python
import functools
import math

import jax
import jax.numpy as jnp
from jax import lax
from jax.experimental import pallas as pl
from jax.experimental.pallas import tpu as pltpu
from jax.sharding import Mesh
from jax.sharding import PartitionSpec as P

D = 4608
FF = 36864
L = 352
TOK = 2 * L
COLS = 2304
HALF = COLS // 2
FEAT = 288
W = 128
NC = HALF // W
AXES = ("x", "zl", "y", "zh", "c")
MESH = pl.DeviceIdType.MESH
BOUND = math.sqrt(L * FF * D / 80.0)
NT = (((1,), (1,)), ((), ()))
ROWS = L // 4


def kernel(
    hid_hbm, gt_hbm, g_hbm, other_ref, out_hbm,
    hid, bb, at, gv, gh, rc, rd, ry, r2, rz, tl, ty, tc, tz, tx, sv, cs, co,
    ld_s, lb_s, t_s, sw_s, sw_r, x_s, x_r, az_s, az_r, ay_s, ay_r, ac_s, ac_r,
    g1_s, g2_s, g2_r, g3_s, t1_s, t1_r, t2_s, t4_s, t4_r, c_s, c_r, o_s,
):
    x, zl, y, zh, c = (lax.axis_index(a) for a in AXES)
    z = zh * 2 + zl
    xr, xl, xo = (x + 1) % 4, (x + 3) % 4, (x + 2) % 4
    yr, yl, yo = (y + 1) % 4, (y + 3) % 4, (y + 2) % 4

    def dev(nx=None, nz=None, ny=None, nc=None):
        nz = z if nz is None else nz
        return (
            x if nx is None else nx,
            nz % 2,
            y if ny is None else ny,
            nz // 2,
            c if nc is None else nc,
        )

    zpair = zh * 2 + (1 - zl)

    def send(src, dst, ss, rs, to):
        return pltpu.make_async_remote_copy(
            src_ref=src, dst_ref=dst, send_sem=ss, recv_sem=rs,
            device_id=to, device_id_type=MESH,
        )

    keep = zl * HALF
    give = (1 - zl) * HALF

    load_hid = pltpu.make_async_copy(hid_hbm, hid, ld_s.at[0])
    load_g = pltpu.make_async_copy(g_hbm, gv, ld_s.at[1])
    load_hid.start()

    def load_own(k):
        col = pl.multiple_of(keep + k * W, W)
        return pltpu.make_async_copy(
            hid_hbm.at[:, pl.ds(col, W)], bb.at[k, x, zl], lb_s.at[k]
        )

    load_g.start()

    @pl.loop(0, NC)
    def _(k):
        load_own(k).start()

    load_t = pltpu.make_async_copy(gt_hbm, at.at[y, z, c], ld_s.at[2])

    @pl.when(x == y)
    def _():
        load_t.start()

    bar = pltpu.get_barrier_semaphore()
    partners = [dev(nx=v) for v in (xr, xl, xo)]
    partners += [dev(ny=v) for v in (yr, yl, yo)]
    partners += [dev(nz=(z + d) % 4) for d in (1, 2, 3)]
    partners += [dev(nc=1 - c)]
    for to in partners:
        pl.semaphore_signal(bar, inc=1, device_id=to, device_id_type=MESH)

    @pl.when(x != y)
    def _():
        pl.semaphore_signal(bar, inc=1, device_id=dev(nx=y, ny=x), device_id_type=MESH)

    pl.semaphore_wait(bar, len(partners) + (x != y).astype(jnp.int32))

    def t_copy():
        return send(gt_hbm, at.at[x, z, c], t_s.at[0], t_s.at[1], dev(nx=y, ny=x))

    @pl.when(x != y)
    def _():
        t_copy().start()

    load_hid.wait()

    def swap(k):
        col = pl.multiple_of(give + k * W, W)
        return send(
            hid.at[:, pl.ds(col, W)], bb.at[k, x, zl], sw_s.at[k], sw_r.at[k],
            dev(nz=zpair),
        )

    for k in range(3):
        swap(k).start()

    def x_copies(k):
        return (
            send(bb.at[k, x], bb.at[k, x], x_s.at[0, k], x_r.at[0, k], dev(nx=xr)),
            send(bb.at[k, x], bb.at[k, x], x_s.at[1, k], x_r.at[1, k], dev(nx=xl)),
        )

    def f_copies(k):
        return (
            send(bb.at[k, xl, 0], bb.at[k, xl, 0], x_s.at[2, k], x_r.at[2, k], dev(nx=xr)),
            send(bb.at[k, xr, 1], bb.at[k, xr, 1], x_s.at[3, k], x_r.at[3, k], dev(nx=xl)),
        )

    def send_x(k):
        load_own(k).wait()
        swap(k).wait_recv()
        for copy in x_copies(k):
            copy.start()

    def fwd_x(k):
        for near, copy in zip(x_copies(k), f_copies(k)):
            near.wait_recv()
            copy.start()

    def far_x(k):
        for copy in f_copies(k):
            copy.wait_recv()

    @pl.loop(0, 2)
    def _(e):
        rows = pl.ds(pl.multiple_of(e * L, 32), L)
        h = hid[rows, :]
        gh[e, 0] = lax.dot_general(h, h, NT, preferred_element_type=jnp.float32)

    load_g.wait()

    @pl.loop(0, 2)
    def _(e):
        rows = pl.ds(pl.multiple_of(e * L, 32), L)
        g = gv[rows, :]
        gh[e, 1] = lax.dot_general(g, g, NT, preferred_element_type=jnp.float32)

    g1 = send(gh.at[1 - c], rc, g1_s.at[0], g1_s.at[1], dev(nc=1 - c))
    g1.start()

    send_x(0)
    swap(3).start()

    @pl.when(x != y)
    def _():
        t_copy().wait()

    @pl.when(x == y)
    def _():
        load_t.wait()

    def z_copy(d):
        return send(
            at.at[y, z, c], at.at[y, z, c], az_s.at[d - 1], az_r.at[d - 1],
            dev(nz=(z + d) % 4),
        )

    for d in (1, 3, 2):
        z_copy(d).start()

    g1.wait()
    rd[...] = gh[c] + rc[...]

    def g2(d):
        to = (y + d) % 4
        rows = pl.ds(pl.multiple_of(to * ROWS, 8), ROWS)
        return send(
            rd.at[:, rows, :], ry.at[d - 1], g2_s.at[d - 1], g2_r.at[d - 1], dev(ny=to)
        )

    for d in (1, 3, 2):
        g2(d).start()

    send_x(1)
    swap(4).start()

    def block(q):
        high = 1 - zl if q < 2 else zl
        low = zl if q % 2 == 0 else 1 - zl
        return high * 2 + low

    top, bottom = pl.ds(0, FEAT // 2), pl.ds(FEAT // 2, FEAT // 2)

    def y_copies(q):
        b = at.at[y, block(q), c]
        return (
            send(b, b, ay_s.at[0, q], ay_r.at[0, q], dev(ny=yr)),
            send(b, b, ay_s.at[1, q], ay_r.at[1, q], dev(ny=yl)),
        )

    def yf_copies(q):
        a = at.at[yl, block(q), c, top]
        b = at.at[yr, block(q), c, bottom]
        return (
            send(a, a, ay_s.at[2, q], ay_r.at[2, q], dev(ny=yr)),
            send(b, b, ay_s.at[3, q], ay_r.at[3, q], dev(ny=yl)),
        )

    def core_copy(q, j):
        b = at.at[(y, yl, yr, yo)[j], block(q), c]
        return send(b, b, ac_s.at[j, q], ac_r.at[j, q], dev(nc=1 - c))

    def own_y(q):
        d = (z - block(q) + 4) % 4

        @pl.when(d != 0)
        def _():
            i = jnp.maximum(d - 1, 0)
            send(
                at.at[y, block(q), c], at.at[y, block(q), c], az_s.at[i], az_r.at[i],
                dev(nz=zpair),
            ).wait_recv()

        for copy in y_copies(q):
            copy.start()
        core_copy(q, 0).start()

    def fwd_y(q):
        for j, (near, copy) in enumerate(zip(y_copies(q), yf_copies(q))):
            near.wait_recv()
            copy.start()
            core_copy(q, 1 + j).start()

    def far_y(q):
        for copy in yf_copies(q):
            copy.wait_recv()
        core_copy(q, 3).start()

    def settle(q):
        for copy in y_copies(q) + yf_copies(q):
            copy.wait_send()
        for j in range(4):
            core_copy(q, j).wait()

    own_y(0)

    for d in (1, 3, 2):
        g2(d).wait()
    mine = pl.ds(pl.multiple_of(y * ROWS, 8), ROWS)
    r2[...] = rd[:, mine, :] + ry[0] + ry[1] + ry[2]
    g3 = send(r2, rz, g3_s.at[0], g3_s.at[1], dev(nz=(z + 2) % 4))
    g3.start()

    send_x(2)
    swap(5).start()

    g3.wait()
    total = r2[...] + rz[...]
    part = jnp.sum(total[0] * total[1])
    lane = lax.broadcasted_iota(jnp.int32, (8, W), 1)
    example = (x * 2 + zl) * 2 + c
    other = jnp.where(c == 0, other_ref[0], other_ref[1])
    tile = jnp.where(lane == example * 4 + y, part, 0.0)
    tl[0] = tile + jnp.where((lane == 64 + example) & (y == 0), other, 0.0)

    def t1(d):
        return send(
            tl.at[0], ty.at[d - 1], t1_s.at[d - 1], t1_r.at[d - 1], dev(ny=(y + d) % 4)
        )

    for d in (1, 3, 2):
        t1(d).start()

    fwd_x(0)

    for d in (1, 3, 2):
        t1(d).wait()
    tl[1] = tl[0] + ty[0] + ty[1] + ty[2]
    t2 = send(tl.at[1], tc, t2_s.at[0], t2_s.at[1], dev(nc=1 - c))
    t2.start()
    t2.wait()
    tl[2] = tl[1] + tc[...]
    t3 = send(tl.at[2], tz, t2_s.at[2], t2_s.at[3], dev(nz=zpair))
    t3.start()
    t3.wait()
    tl[3] = tl[2] + tz[...]

    def t4(d):
        return send(
            tl.at[3], tx.at[d - 1], t4_s.at[d - 1], t4_r.at[d - 1], dev(nx=(x + d) % 4)
        )

    for d in (1, 3, 2):
        t4(d).start()

    own_y(1)
    send_x(3)
    swap(6).start()
    fwd_y(0)
    fwd_x(1)
    send_x(4)
    swap(7).start()

    for d in (1, 3, 2):
        t4(d).wait()
    full = (tl[3] + tx[0] + tx[1] + tx[2])[0:1]
    row = lax.broadcasted_iota(jnp.int32, (1, W), 1)
    token = lax.broadcasted_iota(jnp.int32, (1, TOK), 1)
    for g in range(8):
        pair = []
        for e in (2 * g, 2 * g + 1):
            layer = jnp.sum(
                jnp.where((row >= 4 * e) & (row < 4 * e + 4), full, 0.0), axis=1, keepdims=True
            )
            rest = jnp.sum(jnp.where(row == 64 + e, full, 0.0), axis=1, keepdims=True)
            pair.append(jnp.minimum(1.0, BOUND / jnp.sqrt(rest + layer)))
        sv[g] = jnp.where(token < L, pair[0], pair[1])

    fwd_y(1)
    far_y(0)
    fwd_x(2)
    own_y(2)
    send_x(5)
    swap(8).start()
    far_y(1)
    fwd_x(3)

    def scale(q):
        settle(q)

        @pl.loop(0, 8)
        def _(i):
            yy, cc = i // 2, i % 2
            s = sv[yy * 2 + block(q) % 2]
            b = at[yy, block(q), cc].astype(jnp.float32)
            at[yy, block(q), cc] = (b * s).astype(jnp.bfloat16)

    def multiply(k, high, dst):
        @pl.loop(0, 2)
        def _(cc):
            acc = None
            for xs in range(4):
                for zs in range(2):
                    p = jnp.dot(
                        at[xs, high * 2 + zs, cc], bb[k, xs, zs],
                        preferred_element_type=jnp.float32,
                    )
                    acc = p if acc is None else acc + p
            dst[k, pl.ds(pl.multiple_of(cc * FEAT, 32), FEAT), :] = acc

    def out_cols(k):
        return out_hbm.at[:, pl.ds(pl.multiple_of(keep + k * W, W), W)]

    def c_copy(k):
        return send(cs.at[k], out_cols(k), c_s.at[k], c_r.at[k], dev(nz=zpair))

    def o_copy(k):
        return pltpu.make_async_copy(co.at[k], out_cols(k), o_s.at[k])

    def give_out(k):
        multiply(k, 1 - zl, cs)
        c_copy(k).start()

    def keep_out(k):
        multiply(k, zl, co)
        o_copy(k).start()

    for d in (1, 3, 2):
        z_copy(d).wait_send()
    scale(0)
    scale(1)

    far_x(0)
    give_out(0)
    own_y(3)
    fwd_y(2)
    far_x(1)
    give_out(1)
    send_x(6)
    fwd_x(4)
    fwd_y(3)
    far_y(2)
    far_x(2)
    give_out(2)
    far_y(3)
    scale(2)
    scale(3)

    @pl.loop(3, NC)
    def _(k):
        @pl.when(k + 4 < NC)
        def _():
            send_x(k + 4)

        @pl.when(k + 2 < NC)
        def _():
            fwd_x(k + 2)

        far_x(k)
        give_out(k)

        @pl.when(k < 6)
        def _():
            keep_out(k - 3)

        keep_out(k)

    @pl.loop(0, NC)
    def _(k):
        swap(k).wait_send()
        for copy in x_copies(k) + f_copies(k):
            copy.wait_send()
        o_copy(k).wait()
        c_copy(k).wait()


def on_device(hidden_act, out_grad, other_sq):
    dma = pltpu.SemaphoreType.DMA
    f32, bf16 = jnp.float32, jnp.bfloat16
    anywhere = pl.BlockSpec(memory_space=pl.ANY)
    return pl.pallas_call(
        kernel,
        out_shape=jax.ShapeDtypeStruct((D // 8, COLS), f32),
        in_specs=[anywhere, anywhere, anywhere, pl.BlockSpec(memory_space=pltpu.SMEM)],
        out_specs=anywhere,
        scratch_shapes=[
            pltpu.VMEM((TOK, COLS), bf16),
            pltpu.VMEM((NC, 4, 2, TOK, W), bf16),
            pltpu.VMEM((4, 4, 2, FEAT, TOK), bf16),
            pltpu.VMEM((TOK, FEAT), bf16),
            pltpu.VMEM((2, 2, L, L), f32),
            pltpu.VMEM((2, L, L), f32),
            pltpu.VMEM((2, L, L), f32),
            pltpu.VMEM((3, 2, ROWS, L), f32),
            pltpu.VMEM((2, ROWS, L), f32),
            pltpu.VMEM((2, ROWS, L), f32),
            pltpu.VMEM((4, 8, W), f32),
            pltpu.VMEM((3, 8, W), f32),
            pltpu.VMEM((8, W), f32),
            pltpu.VMEM((8, W), f32),
            pltpu.VMEM((3, 8, W), f32),
            pltpu.VMEM((8, 1, TOK), f32),
            pltpu.VMEM((NC, 2 * FEAT, W), f32),
            pltpu.VMEM((NC, 2 * FEAT, W), f32),
            dma((3,)), dma((NC,)), dma((2,)), dma((NC,)), dma((NC,)),
            dma((4, NC)), dma((4, NC)), dma((3,)), dma((3,)),
            dma((4, 4)), dma((4, 4)), dma((4, 4)), dma((4, 4)),
            dma((2,)), dma((3,)), dma((3,)), dma((2,)),
            dma((3,)), dma((3,)), dma((4,)), dma((3,)), dma((3,)),
            dma((NC,)), dma((NC,)), dma((NC,)),
        ],
        compiler_params=pltpu.CompilerParams(
            collective_id=0, has_side_effects=True, vmem_limit_bytes=60 * 2**20
        ),
    )(hidden_act, out_grad.T, out_grad, other_sq)


def solution(mesh):
    torus = Mesh(mesh.devices.reshape(4, 2, 4, 2, 2), AXES)
    dp, tensor = ("x", "zl"), ("y", "zh", "c")
    return jax.shard_map(
        on_device,
        mesh=torus,
        in_specs=(P(dp, tensor), P(dp, tensor), P(dp)),
        out_specs=P(dp, tensor),
        check_vma=False,
    )
```

```python
import functools
import math

import jax
import jax.numpy as jnp
from jax import lax
from jax.experimental import pallas as pl
from jax.experimental.pallas import tpu as pltpu
from jax.sharding import Mesh
from jax.sharding import PartitionSpec as P

D = 4608
FF = 36864
L = 352
TOK = 2 * L
COLS = 2304
HALF = COLS // 2
FEAT = 288
SUB = FEAT // 2
W = 128
NC = HALF // W
AXES = ("x", "zl", "y", "zh", "c")
MESH = pl.DeviceIdType.MESH
BOUND = math.sqrt(L * FF * D / 80.0)
NT = (((1,), (1,)), ((), ()))
PACK = 672
ROWS = PACK // 4


def kernel(
    hid_hbm, gt_hbm, g_hbm, other_ref, out_hbm,
    hid, bb, at, tb, gv, gh, rc, rd, ry, r2, rz, tl, ty, tc, tz, tx, sv, cs, co, cl,
    ld_s, lb_s, t_s, t_r, u_s, u_r, sw_s, sw_r, x_s, x_r, az_s, az_r, ay_s, ay_r, ac_s, ac_r,
    g1_s, g2_s, g2_r, g3_s, t1_s, t1_r, t2_s, t4_s, t4_r, c_s, c_r, o_s,
):
    x, zl, y, zh, c = (lax.axis_index(a) for a in AXES)
    z = zh * 2 + zl
    xr, xl, xo = (x + 1) % 4, (x + 3) % 4, (x + 2) % 4
    yr, yl, yo = (y + 1) % 4, (y + 3) % 4, (y + 2) % 4

    def dev(nx=None, nz=None, ny=None, nc=None):
        nz = z if nz is None else nz
        return (
            x if nx is None else nx,
            nz % 2,
            y if ny is None else ny,
            nz // 2,
            c if nc is None else nc,
        )

    zpair = zh * 2 + (1 - zl)

    def send(src, dst, ss, rs, to):
        return pltpu.make_async_remote_copy(
            src_ref=src, dst_ref=dst, send_sem=ss, recv_sem=rs,
            device_id=to, device_id_type=MESH,
        )

    keep = zl * HALF
    give = (1 - zl) * HALF

    load_hid = pltpu.make_async_copy(hid_hbm, hid, ld_s.at[0])
    load_g = pltpu.make_async_copy(g_hbm, gv, ld_s.at[1])
    load_hid.start()

    def load_own(k):
        col = pl.multiple_of(keep + k * W, W)
        return pltpu.make_async_copy(
            hid_hbm.at[:, pl.ds(col, W)], bb.at[k, x, zl], lb_s.at[k]
        )

    load_g.start()

    @pl.loop(0, NC)
    def _(k):
        load_own(k).start()

    def rows_of(j):
        return pl.ds(pl.multiple_of(j * SUB, 16), SUB)

    def t_copy(r):
        return send(
            gt_hbm.at[pl.ds(r * SUB, SUB)], tb.at[y % 2], t_s.at[r], t_r.at[y % 2],
            dev(ny=2 * c + r, nc=y // 2),
        )

    def t_here(r):
        return pltpu.make_async_copy(
            gt_hbm.at[pl.ds(r * SUB, SUB)], tb.at[y % 2], t_r.at[y % 2]
        )

    def u_copy(i):
        return send(
            tb.at[i], at.at[x, z, rows_of(y)], u_s.at[i], u_r.at[x % 2],
            dev(nx=2 * c + i, nc=x // 2),
        )

    bar = pltpu.get_barrier_semaphore()
    partners = [dev(nx=v) for v in (xr, xl, xo)]
    partners += [dev(ny=v) for v in (yr, yl, yo)]
    partners += [dev(nz=(z + d) % 4) for d in (1, 2, 3)]
    partners += [dev(nc=1 - c)]
    for to in partners:
        pl.semaphore_signal(bar, inc=1, device_id=to, device_id_type=MESH)

    count = len(partners)
    for i in range(2):
        for away, to in (
            (2 * c + i != y, dev(ny=2 * c + i, nc=y // 2)),
            (2 * c + i != x, dev(nx=2 * c + i, nc=x // 2)),
        ):
            count = count + away.astype(jnp.int32)

            @pl.when(away)
            def _():
                pl.semaphore_signal(bar, inc=1, device_id=to, device_id_type=MESH)

    pl.semaphore_wait(bar, count)

    for r in range(2):

        @pl.when(2 * c + r != y)
        def _():
            t_copy(r).start()

        @pl.when(2 * c + r == y)
        def _():
            t_here(r).start()

    def swap(k):
        col = pl.multiple_of(give + k * W, W)
        return send(
            hid.at[:, pl.ds(col, W)], bb.at[k, x, zl], sw_s.at[k], sw_r.at[k],
            dev(nz=zpair),
        )

    def x_copies(k):
        own, swapped = bb.at[k, x, zl], bb.at[k, x, 1 - zl]
        return (
            send(own, own, x_s.at[0, k], x_r.at[0, k], dev(nx=xr)),
            send(own, own, x_s.at[1, k], x_r.at[1, k], dev(nx=xl)),
            send(swapped, swapped, x_s.at[2, k], x_r.at[2, k], dev(nx=xr)),
            send(swapped, swapped, x_s.at[3, k], x_r.at[3, k], dev(nx=xl)),
        )

    def f_copies(k):
        a, b = bb.at[k, xl, 0], bb.at[k, xr, 1]
        return (
            send(a, a, x_s.at[4, k], x_r.at[4, k], dev(nx=xr)),
            send(b, b, x_s.at[5, k], x_r.at[5, k], dev(nx=xl)),
        )

    def own_x(k):
        load_own(k).wait()
        for copy in x_copies(k)[:2]:
            copy.start()

    def part_x(k):
        swap(k).wait_recv()
        for copy in x_copies(k)[2:]:
            copy.start()

    def fwd_x(k):
        for copy in x_copies(k):
            copy.wait_recv()
        for copy in f_copies(k):
            copy.start()

    def far_x(k):
        for copy in f_copies(k):
            copy.wait_recv()

    load_hid.wait()
    swap(0).start()
    swap(1).start()
    own_x(0)

    def pack(e, kind, gram):
        gh[e, kind, 0:352, :] = gram[:, 0:128]
        gh[e, kind, 352:576, :] = gram[128:352, 128:256]
        gh[e, kind, 576:672, :] = jnp.zeros((96, W), jnp.float32)
        gh[e, kind, 576:672, 0:96] = gram[256:352, 256:352]

    @pl.loop(0, 2)
    def _(e):
        rows = pl.ds(pl.multiple_of(e * L, 32), L)
        h = hid[rows, :]
        pack(e, 0, lax.dot_general(h, h, NT, preferred_element_type=jnp.float32))

    load_g.wait()

    @pl.loop(0, 2)
    def _(e):
        rows = pl.ds(pl.multiple_of(e * L, 32), L)
        g = gv[rows, :]
        pack(e, 1, lax.dot_general(g, g, NT, preferred_element_type=jnp.float32))

    g1 = send(gh.at[1 - c], rc, g1_s.at[0], g1_s.at[1], dev(nc=1 - c))
    g1.start()

    zr, zb = (z + 1) % 4, (z + 3) % 4

    def piece(i, zz, yy):
        return at.at[2 * c + i, zz, rows_of(yy)]

    def z_copies(i):
        b = piece(i, z, y)
        return (
            send(b, b, az_s.at[i], az_r.at[i], dev(nz=zr)),
            send(b, b, az_s.at[2 + i], az_r.at[2 + i], dev(nz=zb)),
        )

    def zf_copies():
        a, b = piece(0, zb, y), piece(1, zr, y)
        return (
            send(a, a, az_s.at[4], az_r.at[4], dev(nz=zr)),
            send(b, b, az_s.at[5], az_r.at[5], dev(nz=zb)),
        )

    middle = zl != zh
    inner = z // 2 * 2 + (1 - zl)
    outer = (z + 2 * zl + 3) % 4
    across = (z + 2) % 4

    def block(q):
        there = (z, inner, outer, across)[q]
        return jnp.where(middle, there, (outer, across, z, inner)[q])

    def y_copies(q, i):
        b = piece(i, block(q), y)
        return (
            send(b, b, ay_s.at[i, q], ay_r.at[i, q], dev(ny=yr)),
            send(b, b, ay_s.at[2 + i, q], ay_r.at[2 + i, q], dev(ny=yl)),
        )

    def yf_copies(q):
        a, b = piece(0, block(q), yl), piece(1, block(q), yr)
        return (
            send(a, a, ay_s.at[4, q], ay_r.at[4, q], dev(ny=yr)),
            send(b, b, ay_s.at[5, q], ay_r.at[5, q], dev(ny=yl)),
        )

    def core_copy(q, j):
        b = at.at[pl.ds(2 * c, 2), block(q), rows_of((y, yl, yr, yo)[j])]
        return send(b, b, ac_s.at[j, q], ac_r.at[j, q], dev(nc=1 - c))

    def own_y(q):
        for i in range(2):
            for copy in y_copies(q, i):
                copy.start()
        core_copy(q, 0).start()

    def fwd_y(q):
        y_copies(q, 0)[0].wait_recv()
        yf_copies(q)[0].start()
        y_copies(q, 1)[1].wait_recv()
        yf_copies(q)[1].start()
        y_copies(q, 1)[0].wait_recv()
        core_copy(q, 1).start()
        y_copies(q, 0)[1].wait_recv()
        core_copy(q, 2).start()

    def far_y(q):
        for copy in yf_copies(q):
            copy.wait_recv()
        core_copy(q, 3).start()

    def settle(q):
        for copy in y_copies(q, 0) + y_copies(q, 1) + yf_copies(q):
            copy.wait_send()
        for j in range(4):
            core_copy(q, j).wait()

    def scale(q):
        settle(q)

        @pl.loop(0, 8)
        def _(i):
            xs = i // 2
            rows = pl.ds(pl.multiple_of(i % 2 * FEAT, 32), FEAT)
            s = sv[xs * 2 + block(q) % 2]
            b = at[xs, block(q), rows].astype(jnp.float32)
            at[xs, block(q), rows] = (b * s).astype(jnp.bfloat16)

    def g2(d):
        to = (y + d) % 4
        rows = pl.ds(pl.multiple_of(to * ROWS, 8), ROWS)
        return send(
            rd.at[:, rows, :], ry.at[d - 1], g2_s.at[d - 1], g2_r.at[d - 1], dev(ny=to)
        )

    part_x(0)
    swap(2).start()
    swap(3).start()
    for i in range(2):
        pltpu.make_async_copy(gt_hbm.at[pl.ds(0, SUB)], tb.at[i], t_r.at[i]).wait()

    for i in range(2):
        far_plane = 2 * c + i != x

        @pl.when(far_plane)
        def _():
            u_copy(i).start()

        @pl.when(jnp.logical_not(far_plane))
        def _():
            at[x, z, rows_of(y)] = tb[i]

    own_x(1)
    g1.wait()
    rd[...] = gh[c] + rc[...]
    for d in (2, 1, 3):
        g2(d).start()
    part_x(1)
    own_x(2)

    for i in range(2):

        @pl.when(2 * c + i != x)
        def _():
            send(
                tb.at[i], at.at[2 * c + i, z, rows_of(y)], u_s.at[i], u_r.at[i],
                dev(nx=2 * c + i, nc=x // 2),
            ).wait_recv()

        for copy in z_copies(i):
            copy.start()

        @pl.when(middle)
        def _():
            for copy in y_copies(0, i):
                copy.start()

    @pl.when(middle)
    def _():
        core_copy(0, 0).start()

    own_x(3)
    fwd_x(0)
    part_x(2)

    for d in (2, 1, 3):
        g2(d).wait()
    mine = pl.ds(pl.multiple_of(y * ROWS, 8), ROWS)
    r2[...] = rd[:, mine, :] + ry[0] + ry[1] + ry[2]
    g3 = send(r2, rz, g3_s.at[0], g3_s.at[1], dev(nz=across))
    g3.start()

    z_copies(0)[0].wait_recv()
    zf_copies()[0].start()
    z_copies(0)[1].wait_recv()
    z_copies(1)[1].wait_recv()
    zf_copies()[1].start()
    z_copies(1)[0].wait_recv()
    swap(4).start()

    @pl.when(jnp.logical_not(middle))
    def _():
        own_y(0)

    part_x(3)
    fwd_x(1)
    own_x(4)
    g3.wait()
    total = r2[...] + rz[...]
    at_row = lax.broadcasted_iota(jnp.int32, (ROWS, W), 0) + y * ROWS
    at_lane = lax.broadcasted_iota(jnp.int32, (ROWS, W), 1)
    tile_of = (at_row >= 352).astype(jnp.int32) + (at_row >= 576).astype(jnp.int32)
    over = at_row - jnp.where(tile_of == 0, 0, jnp.where(tile_of == 1, 352, 576)) - at_lane
    weight = jnp.where(over > 0, 2.0, jnp.where(over == 0, 1.0, 0.0))
    part = jnp.sum(total[0] * total[1] * weight)
    lane = lax.broadcasted_iota(jnp.int32, (8, W), 1)
    example = (x * 2 + zl) * 2 + c
    other = jnp.where(c == 0, other_ref[0], other_ref[1])
    tile = jnp.where(lane == example * 4 + y, part, 0.0)
    tl[0] = tile + jnp.where((lane == 64 + example) & (y == 0), other, 0.0)

    def t1(d):
        return send(
            tl.at[0], ty.at[d - 1], t1_s.at[d - 1], t1_r.at[d - 1], dev(ny=(y + d) % 4)
        )

    for d in (2, 1, 3):
        t1(d).start()

    @pl.when(middle)
    def _():
        own_y(1)

    for copy in zf_copies():
        copy.wait_recv()

    @pl.when(jnp.logical_not(middle))
    def _():
        own_y(1)

    swap(5).start()
    fwd_y(0)

    for d in (2, 1, 3):
        t1(d).wait()
    tl[1] = tl[0] + ty[0] + ty[1] + ty[2]
    t2 = send(tl.at[1], tc, t2_s.at[0], t2_s.at[1], dev(nc=1 - c))
    t2.start()
    t2.wait()
    tl[2] = tl[1] + tc[...]
    t3 = send(tl.at[2], tz, t2_s.at[2], t2_s.at[3], dev(nz=zpair))
    t3.start()
    t3.wait()
    tl[3] = tl[2] + tz[...]

    def t4(d):
        return send(
            tl.at[3], tx.at[d - 1], t4_s.at[d - 1], t4_r.at[d - 1], dev(nx=(x + d) % 4)
        )

    for d in (2, 1, 3):
        t4(d).start()

    fwd_x(2)
    part_x(4)
    own_x(5)
    swap(6).start()
    fwd_y(1)
    own_y(2)
    part_x(5)
    swap(7).start()
    swap(8).start()
    far_y(0)
    own_x(6)
    own_y(3)

    for d in (2, 1, 3):
        t4(d).wait()
    full = (tl[3] + tx[0] + tx[1] + tx[2])[0:1]
    row = lax.broadcasted_iota(jnp.int32, (1, W), 1)
    token = lax.broadcasted_iota(jnp.int32, (1, TOK), 1)
    for g in range(8):
        pair = []
        for e in (2 * g, 2 * g + 1):
            layer = jnp.sum(
                jnp.where((row >= 4 * e) & (row < 4 * e + 4), full, 0.0), axis=1, keepdims=True
            )
            rest = jnp.sum(jnp.where(row == 64 + e, full, 0.0), axis=1, keepdims=True)
            pair.append(jnp.minimum(1.0, BOUND / jnp.sqrt(rest + layer)))
        sv[g] = jnp.where(token < L, pair[0], pair[1])

    for i in range(2):

        @pl.when(2 * c + i != y)
        def _():
            t_copy(i).wait_send()

        @pl.when(2 * c + i != x)
        def _():
            u_copy(i).wait_send()

    for copy in z_copies(0) + z_copies(1) + zf_copies():
        copy.wait_send()
    far_y(1)
    fwd_x(3)
    scale(0)
    scale(1)

    def multiply(high, rhs, put):
        @pl.loop(0, 2)
        def _(cc):
            rows = pl.ds(pl.multiple_of(cc * FEAT, 32), FEAT)
            acc = None
            for xs in range(4):
                for zs in range(2):
                    p = jnp.dot(
                        at[xs, high * 2 + zs, rows], rhs(xs, zs),
                        preferred_element_type=jnp.float32,
                    )
                    acc = p if acc is None else acc + p
            put(rows, acc)

    def out_cols(k, width):
        return out_hbm.at[:, pl.ds(pl.multiple_of(keep + k * W, W), width)]

    def c_copy(k):
        return send(cs.at[k], out_cols(k, W), c_s.at[k], c_r.at[k], dev(nz=zpair))

    def o_copy(i):
        return pltpu.make_async_copy(co.at[i], out_cols(2 * i, 2 * W), o_s.at[i])

    def give_out(k):
        def put(rows, acc):
            cs[k, rows, :] = acc

        multiply(1 - zl, lambda xs, zs: bb[k, xs, zs], put)
        c_copy(k).start()

    def keep_out(i):
        def put(rows, acc):
            co[i, rows, :] = acc

        def rhs(xs, zs):
            return jnp.concatenate([bb[2 * i, xs, zs], bb[2 * i + 1, xs, zs]], axis=1)

        multiply(zl, rhs, put)
        o_copy(i).start()

    last_copy = pltpu.make_async_copy(cl, out_cols(NC - 1, W), o_s.at[4])

    def keep_last():
        def put(rows, acc):
            cl[rows, :] = acc

        multiply(zl, lambda xs, zs: bb[NC - 1, xs, zs], put)
        last_copy.start()

    def serve_x(k):
        @pl.when(k + 5 < NC)
        def _():
            own_x(k + 5)

        @pl.when(k + 4 < NC)
        def _():
            part_x(k + 4)

        @pl.when(k + 2 < NC)
        def _():
            fwd_x(k + 2)

    @pl.loop(0, 5)
    def _(k):
        @pl.when(k >= 2)
        def _():
            serve_x(k)

        far_x(k)
        give_out(k)

        @pl.when(k == 2)
        def _():
            fwd_y(2)

        @pl.when(k == 3)
        def _():
            far_y(2)

    fwd_y(3)
    far_y(3)
    scale(2)
    scale(3)

    @pl.loop(5, NC)
    def _(k):
        serve_x(k)
        far_x(k)
        give_out(k)

        @pl.loop(jnp.where(k == 5, 0, k - 4), jnp.minimum(k - 3, 4))
        def _(i):
            keep_out(i)

    keep_last()

    @pl.loop(0, NC)
    def _(k):
        swap(k).wait_send()
        for copy in x_copies(k) + f_copies(k):
            copy.wait_send()
        c_copy(k).wait()

    @pl.loop(0, 4)
    def _(i):
        o_copy(i).wait()

    last_copy.wait()


def on_device(hidden_act, out_grad, other_sq):
    dma = pltpu.SemaphoreType.DMA
    f32, bf16 = jnp.float32, jnp.bfloat16
    anywhere = pl.BlockSpec(memory_space=pl.ANY)
    return pl.pallas_call(
        kernel,
        out_shape=jax.ShapeDtypeStruct((D // 8, COLS), f32),
        in_specs=[anywhere, anywhere, anywhere, pl.BlockSpec(memory_space=pltpu.SMEM)],
        out_specs=anywhere,
        scratch_shapes=[
            pltpu.VMEM((TOK, COLS), bf16),
            pltpu.VMEM((NC, 4, 2, TOK, W), bf16),
            pltpu.VMEM((4, 4, 2 * FEAT, TOK), bf16),
            pltpu.VMEM((2, SUB, TOK), bf16),
            pltpu.VMEM((TOK, FEAT), bf16),
            pltpu.VMEM((2, 2, PACK, W), f32),
            pltpu.VMEM((2, PACK, W), f32),
            pltpu.VMEM((2, PACK, W), f32),
            pltpu.VMEM((3, 2, ROWS, W), f32),
            pltpu.VMEM((2, ROWS, W), f32),
            pltpu.VMEM((2, ROWS, W), f32),
            pltpu.VMEM((4, 8, W), f32),
            pltpu.VMEM((3, 8, W), f32),
            pltpu.VMEM((8, W), f32),
            pltpu.VMEM((8, W), f32),
            pltpu.VMEM((3, 8, W), f32),
            pltpu.VMEM((8, 1, TOK), f32),
            pltpu.VMEM((NC, 2 * FEAT, W), f32),
            pltpu.VMEM((4, 2 * FEAT, 2 * W), f32),
            pltpu.VMEM((2 * FEAT, W), f32),
            dma((2,)), dma((NC,)), dma((2,)), dma((2,)), dma((2,)), dma((2,)), dma((NC,)), dma((NC,)),
            dma((6, NC)), dma((6, NC)), dma((6,)), dma((6,)),
            dma((6, 4)), dma((6, 4)), dma((4, 4)), dma((4, 4)),
            dma((2,)), dma((3,)), dma((3,)), dma((2,)),
            dma((3,)), dma((3,)), dma((4,)), dma((3,)), dma((3,)),
            dma((NC,)), dma((NC,)), dma((5,)),
        ],
        compiler_params=pltpu.CompilerParams(
            collective_id=0, has_side_effects=True, vmem_limit_bytes=60 * 2**20
        ),
    )(hidden_act, out_grad.T, out_grad, other_sq)


def solution(mesh):
    torus = Mesh(mesh.devices.reshape(4, 2, 4, 2, 2), AXES)
    dp, tensor = ("x", "zl"), ("y", "zh", "c")
    return jax.shard_map(
        on_device,
        mesh=torus,
        in_specs=(P(dp, tensor), P(dp, tensor), P(dp)),
        out_specs=P(dp, tensor),
        check_vma=False,
    )
```

```python
import functools
import math

import jax
import jax.numpy as jnp
from jax import lax
from jax.experimental import pallas as pl
from jax.experimental.pallas import tpu as pltpu
from jax.sharding import Mesh
from jax.sharding import PartitionSpec as P

D = 4608
FF = 36864
L = 352
TOK = 2 * L
COLS = 2304
HALF = COLS // 2
FEAT = 288
SUB = FEAT // 2
W = 128
VMEM_LIMIT = 61_400_000
NC = HALF // W
AXES = ("x", "zl", "y", "zh", "c")
MESH = pl.DeviceIdType.MESH
BOUND = math.sqrt(L * FF * D / 80.0)
NT = (((1,), (1,)), ((), ()))
PACK = 672
ROWS = PACK // 4


def kernel(
    hid_hbm, gt_hbm, other_ref, out,
    hid, bb, at, tb, gv, gh, rc, rd, ry, r2, rz, tl, ty, tc, tz, tx, sv, cs,
    ld_s, lb_s, t_s, t_r, u_s, u_r, sw_s, sw_r, x_s, x_r, az_s, az_r, ay_s, ay_r, ac_s, ac_r,
    g1_s, g2_s, g2_r, g3_s, t1_s, t1_r, t2_s, t4_s, t4_r, c_s, c_r,
):
    x, zl, y, zh, c = (lax.axis_index(a) for a in AXES)
    z = zh * 2 + zl
    xr, xl, xo = (x + 1) % 4, (x + 3) % 4, (x + 2) % 4
    yr, yl, yo = (y + 1) % 4, (y + 3) % 4, (y + 2) % 4

    def dev(nx=None, nz=None, ny=None, nc=None):
        nz = z if nz is None else nz
        return (
            x if nx is None else nx,
            nz % 2,
            y if ny is None else ny,
            nz // 2,
            c if nc is None else nc,
        )

    zpair = zh * 2 + (1 - zl)

    def send(src, dst, ss, rs, to):
        return pltpu.make_async_remote_copy(
            src_ref=src, dst_ref=dst, send_sem=ss, recv_sem=rs,
            device_id=to, device_id_type=MESH,
        )

    keep = zl * HALF
    give = (1 - zl) * HALF

    load_hid = pltpu.make_async_copy(hid_hbm, hid, ld_s.at[0])
    load_g = pltpu.make_async_copy(gt_hbm, gv, ld_s.at[1])
    load_hid.start()

    def load_own(k):
        col = pl.multiple_of(keep + k * W, W)
        return pltpu.make_async_copy(
            hid_hbm.at[:, pl.ds(col, W)], bb.at[k, x, zl], lb_s.at[k]
        )

    load_g.start()

    @pl.loop(0, NC)
    def _(k):
        load_own(k).start()

    def rows_of(j):
        return pl.ds(pl.multiple_of(j * SUB, 16), SUB)

    def t_copy(r):
        return send(
            gt_hbm.at[pl.ds(r * SUB, SUB)], tb.at[y % 2], t_s.at[r], t_r.at[y % 2],
            dev(ny=2 * c + r, nc=y // 2),
        )

    def t_here(r):
        return pltpu.make_async_copy(
            gt_hbm.at[pl.ds(r * SUB, SUB)], tb.at[y % 2], t_r.at[y % 2]
        )

    def u_copy(i):
        return send(
            tb.at[i], at.at[x, z, rows_of(y)], u_s.at[i], u_r.at[x % 2],
            dev(nx=2 * c + i, nc=x // 2),
        )

    bar = pltpu.get_barrier_semaphore()
    partners = [dev(nx=v) for v in (xr, xl, xo)]
    partners += [dev(ny=v) for v in (yr, yl, yo)]
    partners += [dev(nz=(z + d) % 4) for d in (1, 2, 3)]
    partners += [dev(nc=1 - c)]
    for to in partners:
        pl.semaphore_signal(bar, inc=1, device_id=to, device_id_type=MESH)

    count = len(partners)
    for i in range(2):
        for away, to in (
            (2 * c + i != y, dev(ny=2 * c + i, nc=y // 2)),
            (2 * c + i != x, dev(nx=2 * c + i, nc=x // 2)),
        ):
            count = count + away.astype(jnp.int32)

            @pl.when(away)
            def _():
                pl.semaphore_signal(bar, inc=1, device_id=to, device_id_type=MESH)

    pl.semaphore_wait(bar, count)

    for r in range(2):

        @pl.when(2 * c + r != y)
        def _():
            t_copy(r).start()

        @pl.when(2 * c + r == y)
        def _():
            t_here(r).start()

    def swap(k):
        col = pl.multiple_of(give + k * W, W)
        return send(
            hid.at[:, pl.ds(col, W)], bb.at[k, x, zl], sw_s.at[k], sw_r.at[k],
            dev(nz=zpair),
        )

    def x_copies(k):
        own, swapped = bb.at[k, x, zl], bb.at[k, x, 1 - zl]
        return (
            send(own, own, x_s.at[0, k], x_r.at[0, k], dev(nx=xr)),
            send(own, own, x_s.at[1, k], x_r.at[1, k], dev(nx=xl)),
            send(swapped, swapped, x_s.at[2, k], x_r.at[2, k], dev(nx=xr)),
            send(swapped, swapped, x_s.at[3, k], x_r.at[3, k], dev(nx=xl)),
        )

    def f_copies(k):
        a, b = bb.at[k, xl, 0], bb.at[k, xr, 1]
        return (
            send(a, a, x_s.at[4, k], x_r.at[4, k], dev(nx=xr)),
            send(b, b, x_s.at[5, k], x_r.at[5, k], dev(nx=xl)),
        )

    def own_x(k):
        load_own(k).wait()
        for copy in x_copies(k)[:2]:
            copy.start()

    def part_x(k):
        swap(k).wait_recv()
        for copy in x_copies(k)[2:]:
            copy.start()

    def fwd_x(k):
        for copy in x_copies(k):
            copy.wait_recv()
        for copy in f_copies(k):
            copy.start()

    def far_x(k):
        for copy in f_copies(k):
            copy.wait_recv()

    load_hid.wait()
    swap(0).start()
    swap(1).start()
    own_x(0)
    own_x(1)

    def pack(e, kind, gram):
        gh[e, kind, 0:352, :] = gram[:, 0:128]
        gh[e, kind, 352:576, :] = gram[128:352, 128:256]
        gh[e, kind, 576:672, :] = jnp.zeros((96, W), jnp.float32)
        gh[e, kind, 576:672, 0:96] = gram[256:352, 256:352]

    @pl.loop(0, 2)
    def _(e):
        rows = pl.ds(pl.multiple_of(e * L, 32), L)
        h = hid[rows, :]
        pack(e, 0, lax.dot_general(h, h, NT, preferred_element_type=jnp.float32))

    load_g.wait()
    turned = jnp.transpose(gv[...])
    for e in range(2):
        g = turned[e * L : (e + 1) * L]
        pack(e, 1, lax.dot_general(g, g, NT, preferred_element_type=jnp.float32))

    g1 = send(gh.at[1 - c], rc, g1_s.at[0], g1_s.at[1], dev(nc=1 - c))
    g1.start()

    zr, zb = (z + 1) % 4, (z + 3) % 4

    def piece(i, zz, yy):
        return at.at[2 * c + i, zz, rows_of(yy)]

    def z_copies(i):
        b = piece(i, z, y)
        return (
            send(b, b, az_s.at[i], az_r.at[i], dev(nz=zr)),
            send(b, b, az_s.at[2 + i], az_r.at[2 + i], dev(nz=zb)),
        )

    def zf_copies():
        a, b = piece(0, zb, y), piece(1, zr, y)
        return (
            send(a, a, az_s.at[4], az_r.at[4], dev(nz=zr)),
            send(b, b, az_s.at[5], az_r.at[5], dev(nz=zb)),
        )

    middle = zl != zh
    inner = z // 2 * 2 + (1 - zl)
    outer = (z + 2 * zl + 3) % 4
    across = (z + 2) % 4

    def block(q):
        there = (z, inner, outer, across)[q]
        return jnp.where(middle, there, (outer, across, z, inner)[q])

    def y_copies(q, i):
        b = piece(i, block(q), y)
        return (
            send(b, b, ay_s.at[i, q], ay_r.at[i, q], dev(ny=yr)),
            send(b, b, ay_s.at[2 + i, q], ay_r.at[2 + i, q], dev(ny=yl)),
        )

    def yf_copies(q):
        a, b = piece(0, block(q), yl), piece(1, block(q), yr)
        return (
            send(a, a, ay_s.at[4, q], ay_r.at[4, q], dev(ny=yr)),
            send(b, b, ay_s.at[5, q], ay_r.at[5, q], dev(ny=yl)),
        )

    def core_copy(q, j):
        b = at.at[pl.ds(2 * c, 2), block(q), rows_of((y, yl, yr, yo)[j])]
        return send(b, b, ac_s.at[j, q], ac_r.at[j, q], dev(nc=1 - c))

    def own_y(q):
        for i in range(2):
            for copy in y_copies(q, i):
                copy.start()
        core_copy(q, 0).start()

    def fwd_y(q):
        y_copies(q, 0)[0].wait_recv()
        yf_copies(q)[0].start()
        y_copies(q, 1)[1].wait_recv()
        yf_copies(q)[1].start()
        y_copies(q, 1)[0].wait_recv()
        core_copy(q, 1).start()
        y_copies(q, 0)[1].wait_recv()
        core_copy(q, 2).start()

    def far_y(q):
        for copy in yf_copies(q):
            copy.wait_recv()
        core_copy(q, 3).start()

    def settle(q):
        for copy in y_copies(q, 0) + y_copies(q, 1) + yf_copies(q):
            copy.wait_send()
        for j in range(4):
            core_copy(q, j).wait()

    def scale(q):
        settle(q)

        @pl.loop(0, 8)
        def _(i):
            xs = i // 2
            rows = pl.ds(pl.multiple_of(i % 2 * FEAT, 32), FEAT)
            s = sv[xs * 2 + block(q) % 2]
            b = at[xs, block(q), rows].astype(jnp.float32)
            at[xs, block(q), rows] = (b * s).astype(jnp.bfloat16)

    def g2(d):
        to = (y + d) % 4
        rows = pl.ds(pl.multiple_of(to * ROWS, 8), ROWS)
        return send(
            rd.at[:, rows, :], ry.at[d - 1], g2_s.at[d - 1], g2_r.at[d - 1], dev(ny=to)
        )

    swap(2).start()
    swap(3).start()
    for i in range(2):
        pltpu.make_async_copy(gt_hbm.at[pl.ds(0, SUB)], tb.at[i], t_r.at[i]).wait()

    for i in range(2):
        far_plane = 2 * c + i != x

        @pl.when(far_plane)
        def _():
            u_copy(i).start()

        @pl.when(jnp.logical_not(far_plane))
        def _():
            at[x, z, rows_of(y)] = tb[i]

    part_x(0)
    g1.wait()
    rd[...] = gh[c] + rc[...]
    for d in (2, 1, 3):
        g2(d).start()
    part_x(1)
    own_x(2)

    for i in range(2):

        @pl.when(2 * c + i != x)
        def _():
            send(
                tb.at[i], at.at[2 * c + i, z, rows_of(y)], u_s.at[i], u_r.at[i],
                dev(nx=2 * c + i, nc=x // 2),
            ).wait_recv()

        for copy in z_copies(i):
            copy.start()

        @pl.when(middle)
        def _():
            for copy in y_copies(0, i):
                copy.start()

    @pl.when(middle)
    def _():
        core_copy(0, 0).start()

    own_x(3)
    part_x(2)

    for d in (2, 1, 3):
        g2(d).wait()
    mine = pl.ds(pl.multiple_of(y * ROWS, 8), ROWS)
    r2[...] = rd[:, mine, :] + ry[0] + ry[1] + ry[2]
    g3 = send(r2, rz, g3_s.at[0], g3_s.at[1], dev(nz=across))
    g3.start()

    z_copies(0)[0].wait_recv()
    zf_copies()[0].start()
    z_copies(0)[1].wait_recv()
    z_copies(1)[1].wait_recv()
    zf_copies()[1].start()
    z_copies(1)[0].wait_recv()
    swap(4).start()

    @pl.when(jnp.logical_not(middle))
    def _():
        own_y(0)

    @pl.when(middle)
    def _():
        own_y(1)

    fwd_x(0)
    part_x(3)
    own_x(4)
    fwd_x(1)
    g3.wait()
    total = r2[...] + rz[...]
    at_row = lax.broadcasted_iota(jnp.int32, (ROWS, W), 0) + y * ROWS
    at_lane = lax.broadcasted_iota(jnp.int32, (ROWS, W), 1)
    tile_of = (at_row >= 352).astype(jnp.int32) + (at_row >= 576).astype(jnp.int32)
    over = at_row - jnp.where(tile_of == 0, 0, jnp.where(tile_of == 1, 352, 576)) - at_lane
    weight = jnp.where(over > 0, 2.0, jnp.where(over == 0, 1.0, 0.0))
    part = jnp.sum(total[0] * total[1] * weight)
    lane = lax.broadcasted_iota(jnp.int32, (8, W), 1)
    example = (x * 2 + zl) * 2 + c
    other = jnp.where(c == 0, other_ref[0], other_ref[1])
    tile = jnp.where(lane == example * 4 + y, part, 0.0)
    tl[0] = tile + jnp.where((lane == 64 + example) & (y == 0), other, 0.0)

    def t1(d):
        return send(
            tl.at[0], ty.at[d - 1], t1_s.at[d - 1], t1_r.at[d - 1], dev(ny=(y + d) % 4)
        )

    for d in (2, 1, 3):
        t1(d).start()

    for copy in zf_copies():
        copy.wait_recv()

    @pl.when(jnp.logical_not(middle))
    def _():
        own_y(1)

    swap(5).start()
    fwd_y(0)

    for d in (2, 1, 3):
        t1(d).wait()
    tl[1] = tl[0] + ty[0] + ty[1] + ty[2]
    t2 = send(tl.at[1], tc, t2_s.at[0], t2_s.at[1], dev(nc=1 - c))
    t2.start()
    t2.wait()
    tl[2] = tl[1] + tc[...]
    t3 = send(tl.at[2], tz, t2_s.at[2], t2_s.at[3], dev(nz=zpair))
    t3.start()
    t3.wait()
    tl[3] = tl[2] + tz[...]

    def t4(d):
        return send(
            tl.at[3], tx.at[d - 1], t4_s.at[d - 1], t4_r.at[d - 1], dev(nx=(x + d) % 4)
        )

    for d in (2, 1, 3):
        t4(d).start()

    fwd_x(2)
    part_x(4)
    own_x(5)
    swap(6).start()
    fwd_y(1)
    own_y(2)
    part_x(5)
    own_x(6)
    swap(7).start()
    swap(8).start()
    far_y(0)
    own_y(3)

    for d in (2, 1, 3):
        t4(d).wait()
    full = (tl[3] + tx[0] + tx[1] + tx[2])[0:1]
    row = lax.broadcasted_iota(jnp.int32, (1, W), 1)
    token = lax.broadcasted_iota(jnp.int32, (1, TOK), 1)
    for g in range(8):
        pair = []
        for e in (2 * g, 2 * g + 1):
            layer = jnp.sum(
                jnp.where((row >= 4 * e) & (row < 4 * e + 4), full, 0.0), axis=1, keepdims=True
            )
            rest = jnp.sum(jnp.where(row == 64 + e, full, 0.0), axis=1, keepdims=True)
            pair.append(jnp.minimum(1.0, BOUND / jnp.sqrt(rest + layer)))
        sv[g] = jnp.where(token < L, pair[0], pair[1])

    for i in range(2):

        @pl.when(2 * c + i != y)
        def _():
            t_copy(i).wait_send()

        @pl.when(2 * c + i != x)
        def _():
            u_copy(i).wait_send()

    for copy in z_copies(0) + z_copies(1) + zf_copies():
        copy.wait_send()
    far_y(1)
    fwd_x(3)
    scale(0)
    scale(1)

    def multiply(high, rhs, put):
        @pl.loop(0, 2)
        def _(cc):
            rows = pl.ds(pl.multiple_of(cc * FEAT, 32), FEAT)
            acc = None
            for xs in range(4):
                for zs in range(2):
                    p = jnp.dot(
                        at[xs, high * 2 + zs, rows], rhs(xs, zs),
                        preferred_element_type=jnp.float32,
                    )
                    acc = p if acc is None else acc + p
            put(cc, rows, acc)

    def c_copy(k, cc):
        rows = pl.ds(pl.multiple_of(cc * FEAT, 32), FEAT)
        cols = pl.ds(pl.multiple_of(keep + k * W, W), W)
        return send(
            cs.at[k, rows], out.at[rows, cols], c_s.at[cc, k], c_r.at[cc, k],
            dev(nz=zpair),
        )

    def give_out(k):
        def put(cc, rows, acc):
            cs[k, rows, :] = acc
            c_copy(k, cc).start()

        multiply(1 - zl, lambda xs, zs: bb[k, xs, zs], put)

    def keep_out(i):
        def put(cc, rows, acc):
            out[rows, pl.ds(pl.multiple_of(keep + i * 2 * W, W), 2 * W)] = acc

        def rhs(xs, zs):
            return jnp.concatenate([bb[2 * i, xs, zs], bb[2 * i + 1, xs, zs]], axis=1)

        multiply(zl, rhs, put)

    def keep_last():
        def put(cc, rows, acc):
            out[rows, pl.ds(pl.multiple_of(keep + (NC - 1) * W, W), W)] = acc

        multiply(zl, lambda xs, zs: bb[NC - 1, xs, zs], put)

    def serve_x(k):
        @pl.when(k + 5 < NC)
        def _():
            own_x(k + 5)

        @pl.when(k + 4 < NC)
        def _():
            part_x(k + 4)

        @pl.when(k + 2 < NC)
        def _():
            fwd_x(k + 2)

    @pl.loop(0, 5)
    def _(k):
        far_x(k)
        give_out(k)

        @pl.when(k == 1)
        def _():
            fwd_y(2)

        @pl.when(k >= 2)
        def _():
            serve_x(k)

        @pl.when(k == 3)
        def _():
            fwd_y(3)

    far_y(2)
    far_y(3)
    scale(2)
    scale(3)

    @pl.loop(5, NC)
    def _(k):
        far_x(k)
        give_out(k)

        @pl.loop(jnp.where(k == 5, 0, k - 4), jnp.minimum(k - 3, 4))
        def _(i):
            keep_out(i)

        serve_x(k)

    keep_last()

    @pl.loop(0, NC)
    def _(k):
        swap(k).wait_send()
        for copy in x_copies(k) + f_copies(k):
            copy.wait_send()
        for cc in range(2):
            c_copy(k, cc).wait()


def on_device(hidden_act, out_grad, other_sq):
    dma = pltpu.SemaphoreType.DMA
    f32, bf16 = jnp.float32, jnp.bfloat16
    anywhere = pl.BlockSpec(memory_space=pltpu.HBM)
    return pl.pallas_call(
        kernel,
        out_shape=pltpu.VMEM((D // 8, COLS), f32),
        in_specs=[anywhere, anywhere, pl.BlockSpec(memory_space=pltpu.SMEM)],
        out_specs=pl.BlockSpec(memory_space=pltpu.VMEM),
        scratch_shapes=[
            pltpu.VMEM((TOK, COLS), bf16),
            pltpu.VMEM((NC, 4, 2, TOK, W), bf16),
            pltpu.VMEM((4, 4, 2 * FEAT, TOK), bf16),
            pltpu.VMEM((2, SUB, TOK), bf16),
            pltpu.VMEM((FEAT, TOK), bf16),
            pltpu.VMEM((2, 2, PACK, W), f32),
            pltpu.VMEM((2, PACK, W), f32),
            pltpu.VMEM((2, PACK, W), f32),
            pltpu.VMEM((3, 2, ROWS, W), f32),
            pltpu.VMEM((2, ROWS, W), f32),
            pltpu.VMEM((2, ROWS, W), f32),
            pltpu.VMEM((4, 8, W), f32),
            pltpu.VMEM((3, 8, W), f32),
            pltpu.VMEM((8, W), f32),
            pltpu.VMEM((8, W), f32),
            pltpu.VMEM((3, 8, W), f32),
            pltpu.VMEM((8, 1, TOK), f32),
            pltpu.VMEM((NC, 2 * FEAT, W), f32),
            dma((2,)), dma((NC,)), dma((2,)), dma((2,)), dma((2,)), dma((2,)), dma((NC,)), dma((NC,)),
            dma((6, NC)), dma((6, NC)), dma((6,)), dma((6,)),
            dma((6, 4)), dma((6, 4)), dma((4, 4)), dma((4, 4)),
            dma((2,)), dma((3,)), dma((3,)), dma((2,)),
            dma((3,)), dma((3,)), dma((4,)), dma((3,)), dma((3,)),
            dma((2, NC)), dma((2, NC)),
        ],
        compiler_params=pltpu.CompilerParams(
            collective_id=0, has_side_effects=True, vmem_limit_bytes=VMEM_LIMIT
        ),
    )(hidden_act, out_grad.T, other_sq)


def solution(mesh):
    torus = Mesh(mesh.devices.reshape(4, 2, 4, 2, 2), AXES)
    dp, tensor = ("x", "zl"), ("y", "zh", "c")
    return jax.shard_map(
        on_device,
        mesh=torus,
        in_specs=(P(dp, tensor), P(dp, tensor), P(dp)),
        out_specs=P(dp, tensor),
        check_vma=False,
    )
```

```python
import functools
import math

import jax
import jax.numpy as jnp
from jax import lax
from jax.experimental import pallas as pl
from jax.experimental.pallas import tpu as pltpu
from jax.sharding import Mesh
from jax.sharding import PartitionSpec as P

D = 4608
FF = 36864
L = 352
TOK = 2 * L
COLS = 2304
HALF = COLS // 2
FEAT = 288
SUB = FEAT // 2
W = 128
VMEM_LIMIT = 61_400_000
NC = HALF // W
AXES = ("x", "zl", "y", "zh", "c")
MESH = pl.DeviceIdType.MESH
BOUND = math.sqrt(L * FF * D / 80.0)
NT = (((1,), (1,)), ((), ()))
PACK = 672
ROWS = PACK // 4


def kernel(
    hid_hbm, gt_hbm, other_ref, out,
    hid, bb, at, tb, gv, gh, rc, rd, ry, r2, rz, tl, ty, tc, tz, tx, sv, cs,
    ld_s, lb_s, t_s, t_r, u_s, u_r, sw_s, sw_r, x_s, x_r, az_s, az_r, ay_s, ay_r, ac_s, ac_r,
    g1_s, g2_s, g2_r, g3_s, t1_s, t1_r, t2_s, t4_s, t4_r, c_s, c_r,
):
    x, zl, y, zh, c = (lax.axis_index(a) for a in AXES)
    z = zh * 2 + zl
    xr, xl, xo = (x + 1) % 4, (x + 3) % 4, (x + 2) % 4
    yr, yl, yo = (y + 1) % 4, (y + 3) % 4, (y + 2) % 4

    def dev(nx=None, nz=None, ny=None, nc=None):
        nz = z if nz is None else nz
        return (
            x if nx is None else nx,
            nz % 2,
            y if ny is None else ny,
            nz // 2,
            c if nc is None else nc,
        )

    zpair = zh * 2 + (1 - zl)

    def send(src, dst, ss, rs, to):
        return pltpu.make_async_remote_copy(
            src_ref=src, dst_ref=dst, send_sem=ss, recv_sem=rs,
            device_id=to, device_id_type=MESH,
        )

    keep = zl * HALF
    give = (1 - zl) * HALF

    load_hid = pltpu.make_async_copy(hid_hbm, hid, ld_s.at[0])
    load_g = pltpu.make_async_copy(gt_hbm, gv, ld_s.at[1])
    load_hid.start()

    def load_own(k):
        col = pl.multiple_of(keep + k * W, W)
        return pltpu.make_async_copy(
            hid_hbm.at[:, pl.ds(col, W)], bb.at[k, x, zl], lb_s.at[k]
        )

    load_g.start()

    @pl.loop(0, NC)
    def _(k):
        load_own(k).start()

    def rows_of(j):
        return pl.ds(pl.multiple_of(j * SUB, 16), SUB)

    def t_copy(r):
        return send(
            gt_hbm.at[pl.ds(r * SUB, SUB)], tb.at[y % 2], t_s.at[r], t_r.at[y % 2],
            dev(ny=2 * c + r, nc=y // 2),
        )

    def t_here(r):
        return pltpu.make_async_copy(
            gt_hbm.at[pl.ds(r * SUB, SUB)], tb.at[y % 2], t_r.at[y % 2]
        )

    def u_copy(i):
        return send(
            tb.at[i], at.at[x, z, rows_of(y)], u_s.at[i], u_r.at[x % 2],
            dev(nx=2 * c + i, nc=x // 2),
        )

    bar = pltpu.get_barrier_semaphore()
    partners = [dev(nx=v) for v in (xr, xl, xo)]
    partners += [dev(ny=v) for v in (yr, yl, yo)]
    partners += [dev(nz=(z + d) % 4) for d in (1, 2, 3)]
    partners += [dev(nc=1 - c)]
    for to in partners:
        pl.semaphore_signal(bar, inc=1, device_id=to, device_id_type=MESH)

    count = len(partners)
    for i in range(2):
        for away, to in (
            (2 * c + i != y, dev(ny=2 * c + i, nc=y // 2)),
            (2 * c + i != x, dev(nx=2 * c + i, nc=x // 2)),
        ):
            count = count + away.astype(jnp.int32)

            @pl.when(away)
            def _():
                pl.semaphore_signal(bar, inc=1, device_id=to, device_id_type=MESH)

    pl.semaphore_wait(bar, count)

    for r in range(2):

        @pl.when(2 * c + r != y)
        def _():
            t_copy(r).start()

        @pl.when(2 * c + r == y)
        def _():
            t_here(r).start()

    def swap(k):
        col = pl.multiple_of(give + k * W, W)
        return send(
            hid.at[:, pl.ds(col, W)], bb.at[k, x, zl], sw_s.at[k], sw_r.at[k],
            dev(nz=zpair),
        )

    def x_copies(k):
        own, swapped = bb.at[k, x, zl], bb.at[k, x, 1 - zl]
        return (
            send(own, own, x_s.at[0, k], x_r.at[0, k], dev(nx=xr)),
            send(own, own, x_s.at[1, k], x_r.at[1, k], dev(nx=xl)),
            send(swapped, swapped, x_s.at[2, k], x_r.at[2, k], dev(nx=xr)),
            send(swapped, swapped, x_s.at[3, k], x_r.at[3, k], dev(nx=xl)),
        )

    def f_copies(k):
        a, b = bb.at[k, xl, 0], bb.at[k, xr, 1]
        return (
            send(a, a, x_s.at[4, k], x_r.at[4, k], dev(nx=xr)),
            send(b, b, x_s.at[5, k], x_r.at[5, k], dev(nx=xl)),
        )

    def own_x(k):
        load_own(k).wait()
        for copy in x_copies(k)[:2]:
            copy.start()

    def part_x(k):
        swap(k).wait_recv()
        for copy in x_copies(k)[2:]:
            copy.start()

    def fwd_x(k):
        for copy in x_copies(k):
            copy.wait_recv()
        for copy in f_copies(k):
            copy.start()

    def far_x(k):
        for copy in f_copies(k):
            copy.wait_recv()

    load_hid.wait()
    swap(0).start()
    swap(1).start()
    own_x(0)
    own_x(1)

    def pack(e, kind, gram):
        gh[e, kind, 0:352, :] = gram[:, 0:128]
        gh[e, kind, 352:576, :] = gram[128:352, 128:256]
        gh[e, kind, 576:672, :] = jnp.zeros((96, W), jnp.float32)
        gh[e, kind, 576:672, 0:96] = gram[256:352, 256:352]

    @pl.loop(0, 2)
    def _(e):
        rows = pl.ds(pl.multiple_of(e * L, 32), L)
        h = hid[rows, :]
        pack(e, 0, lax.dot_general(h, h, NT, preferred_element_type=jnp.float32))

    load_g.wait()
    turned = jnp.transpose(gv[...])
    for e in range(2):
        g = turned[e * L : (e + 1) * L]
        pack(e, 1, lax.dot_general(g, g, NT, preferred_element_type=jnp.float32))

    g1 = send(gh.at[1 - c], rc, g1_s.at[0], g1_s.at[1], dev(nc=1 - c))
    g1.start()

    zr, zb = (z + 1) % 4, (z + 3) % 4

    def piece(i, zz, yy):
        return at.at[2 * c + i, zz, rows_of(yy)]

    def z_copies(i):
        b = piece(i, z, y)
        return (
            send(b, b, az_s.at[i], az_r.at[i], dev(nz=zr)),
            send(b, b, az_s.at[2 + i], az_r.at[2 + i], dev(nz=zb)),
        )

    def zf_copies():
        a, b = piece(0, zb, y), piece(1, zr, y)
        return (
            send(a, a, az_s.at[4], az_r.at[4], dev(nz=zr)),
            send(b, b, az_s.at[5], az_r.at[5], dev(nz=zb)),
        )

    middle = zl != zh
    inner = z // 2 * 2 + (1 - zl)
    outer = (z + 2 * zl + 3) % 4
    across = (z + 2) % 4

    def block(q):
        there = (z, inner, outer, across)[q]
        return jnp.where(middle, there, (outer, across, z, inner)[q])

    def y_copies(q, i):
        b = piece(i, block(q), y)
        return (
            send(b, b, ay_s.at[i, q], ay_r.at[i, q], dev(ny=yr)),
            send(b, b, ay_s.at[2 + i, q], ay_r.at[2 + i, q], dev(ny=yl)),
        )

    def yf_copies(q):
        a, b = piece(0, block(q), yl), piece(1, block(q), yr)
        return (
            send(a, a, ay_s.at[4, q], ay_r.at[4, q], dev(ny=yr)),
            send(b, b, ay_s.at[5, q], ay_r.at[5, q], dev(ny=yl)),
        )

    def core_copy(q, j):
        b = at.at[pl.ds(2 * c, 2), block(q), rows_of((y, yl, yr, yo)[j])]
        return send(b, b, ac_s.at[j, q], ac_r.at[j, q], dev(nc=1 - c))

    def own_y(q):
        for i in range(2):
            for copy in y_copies(q, i):
                copy.start()
        core_copy(q, 0).start()

    def fwd_y(q):
        y_copies(q, 0)[0].wait_recv()
        yf_copies(q)[0].start()
        y_copies(q, 1)[1].wait_recv()
        yf_copies(q)[1].start()
        y_copies(q, 1)[0].wait_recv()
        core_copy(q, 1).start()
        y_copies(q, 0)[1].wait_recv()
        core_copy(q, 2).start()

    def far_y(q):
        for copy in yf_copies(q):
            copy.wait_recv()
        core_copy(q, 3).start()

    def settle(q):
        for copy in y_copies(q, 0) + y_copies(q, 1) + yf_copies(q):
            copy.wait_send()
        for j in range(4):
            core_copy(q, j).wait()

    def scale(q):
        settle(q)

        @pl.loop(0, 8)
        def _(i):
            xs = i // 2
            rows = pl.ds(pl.multiple_of(i % 2 * FEAT, 32), FEAT)
            s = sv[xs * 2 + block(q) % 2]
            b = at[xs, block(q), rows].astype(jnp.float32)
            at[xs, block(q), rows] = (b * s).astype(jnp.bfloat16)

    def g2(d):
        to = (y + d) % 4
        rows = pl.ds(pl.multiple_of(to * ROWS, 8), ROWS)
        return send(
            rd.at[:, rows, :], ry.at[d - 1], g2_s.at[d - 1], g2_r.at[d - 1], dev(ny=to)
        )

    swap(2).start()
    swap(3).start()
    for i in range(2):
        pltpu.make_async_copy(gt_hbm.at[pl.ds(0, SUB)], tb.at[i], t_r.at[i]).wait()

    for i in range(2):
        far_plane = 2 * c + i != x

        @pl.when(far_plane)
        def _():
            u_copy(i).start()

        @pl.when(jnp.logical_not(far_plane))
        def _():
            at[x, z, rows_of(y)] = tb[i]

    part_x(0)
    g1.wait()
    rd[...] = gh[c] + rc[...]
    for d in (2, 1, 3):
        g2(d).start()
    part_x(1)
    own_x(2)

    for i in range(2):

        @pl.when(2 * c + i != x)
        def _():
            send(
                tb.at[i], at.at[2 * c + i, z, rows_of(y)], u_s.at[i], u_r.at[i],
                dev(nx=2 * c + i, nc=x // 2),
            ).wait_recv()

        for copy in z_copies(i):
            copy.start()

        @pl.when(middle)
        def _():
            for copy in y_copies(0, i):
                copy.start()

    @pl.when(middle)
    def _():
        core_copy(0, 0).start()

    own_x(3)
    part_x(2)

    for d in (2, 1, 3):
        g2(d).wait()
    mine = pl.ds(pl.multiple_of(y * ROWS, 8), ROWS)
    r2[...] = rd[:, mine, :] + ry[0] + ry[1] + ry[2]
    g3 = send(r2, rz, g3_s.at[0], g3_s.at[1], dev(nz=across))
    g3.start()

    z_copies(0)[0].wait_recv()
    zf_copies()[0].start()
    z_copies(0)[1].wait_recv()
    z_copies(1)[1].wait_recv()
    zf_copies()[1].start()
    z_copies(1)[0].wait_recv()
    swap(4).start()

    @pl.when(jnp.logical_not(middle))
    def _():
        own_y(0)

    @pl.when(middle)
    def _():
        own_y(1)

    fwd_x(0)
    part_x(3)
    own_x(4)
    fwd_x(1)
    g3.wait()
    total = r2[...] + rz[...]
    at_row = lax.broadcasted_iota(jnp.int32, (ROWS, W), 0) + y * ROWS
    at_lane = lax.broadcasted_iota(jnp.int32, (ROWS, W), 1)
    tile_of = (at_row >= 352).astype(jnp.int32) + (at_row >= 576).astype(jnp.int32)
    over = at_row - jnp.where(tile_of == 0, 0, jnp.where(tile_of == 1, 352, 576)) - at_lane
    weight = jnp.where(over > 0, 2.0, jnp.where(over == 0, 1.0, 0.0))
    part = jnp.sum(total[0] * total[1] * weight)
    lane = lax.broadcasted_iota(jnp.int32, (8, W), 1)
    example = (x * 2 + zl) * 2 + c
    other = jnp.where(c == 0, other_ref[0], other_ref[1])
    tile = jnp.where(lane == example * 4 + y, part, 0.0)
    tl[0] = tile + jnp.where((lane == 64 + example) & (y == 0), other, 0.0)

    def t1(d):
        return send(
            tl.at[0], ty.at[d - 1], t1_s.at[d - 1], t1_r.at[d - 1], dev(ny=(y + d) % 4)
        )

    for d in (2, 1, 3):
        t1(d).start()

    for copy in zf_copies():
        copy.wait_recv()

    @pl.when(jnp.logical_not(middle))
    def _():
        own_y(1)

    swap(5).start()
    fwd_y(0)

    for d in (2, 1, 3):
        t1(d).wait()
    tl[1] = tl[0] + ty[0] + ty[1] + ty[2]
    t2 = send(tl.at[1], tc, t2_s.at[0], t2_s.at[1], dev(nc=1 - c))
    t2.start()
    t2.wait()
    tl[2] = tl[1] + tc[...]
    t3 = send(tl.at[2], tz, t2_s.at[2], t2_s.at[3], dev(nz=zpair))
    t3.start()
    t3.wait()
    tl[3] = tl[2] + tz[...]

    def t4(d):
        return send(
            tl.at[3], tx.at[d - 1], t4_s.at[d - 1], t4_r.at[d - 1], dev(nx=(x + d) % 4)
        )

    for d in (2, 1, 3):
        t4(d).start()

    fwd_x(2)
    part_x(4)
    own_x(5)
    swap(6).start()
    fwd_y(1)
    own_y(2)
    part_x(5)
    own_x(6)
    swap(7).start()
    swap(8).start()
    far_y(0)
    own_y(3)

    for d in (2, 1, 3):
        t4(d).wait()
    full = (tl[3] + tx[0] + tx[1] + tx[2])[0:1]
    row = lax.broadcasted_iota(jnp.int32, (1, W), 1)
    token = lax.broadcasted_iota(jnp.int32, (1, TOK), 1)
    for g in range(8):
        pair = []
        for e in (2 * g, 2 * g + 1):
            layer = jnp.sum(
                jnp.where((row >= 4 * e) & (row < 4 * e + 4), full, 0.0), axis=1, keepdims=True
            )
            rest = jnp.sum(jnp.where(row == 64 + e, full, 0.0), axis=1, keepdims=True)
            pair.append(jnp.minimum(1.0, BOUND / jnp.sqrt(rest + layer)))
        sv[g] = jnp.where(token < L, pair[0], pair[1])

    for i in range(2):

        @pl.when(2 * c + i != y)
        def _():
            t_copy(i).wait_send()

        @pl.when(2 * c + i != x)
        def _():
            u_copy(i).wait_send()

    for copy in z_copies(0) + z_copies(1) + zf_copies():
        copy.wait_send()
    far_y(1)
    fwd_x(3)
    scale(0)
    scale(1)

    def multiply(high, rhs, put):
        @pl.loop(0, 2)
        def _(cc):
            rows = pl.ds(pl.multiple_of(cc * FEAT, 32), FEAT)
            acc = None
            for xs in range(4):
                for zs in range(2):
                    p = jnp.dot(
                        at[xs, high * 2 + zs, rows], rhs(xs, zs),
                        preferred_element_type=jnp.float32,
                    )
                    acc = p if acc is None else acc + p
            put(cc, rows, acc)

    def c_copy(k, cc):
        rows = pl.ds(pl.multiple_of(cc * FEAT, 32), FEAT)
        cols = pl.ds(pl.multiple_of(keep + k * W, W), W)
        return send(
            cs.at[k, rows], out.at[rows, cols], c_s.at[cc, k], c_r.at[cc, k],
            dev(nz=zpair),
        )

    def give_out(k):
        def put(cc, rows, acc):
            cs[k, rows, :] = acc
            c_copy(k, cc).start()

        multiply(1 - zl, lambda xs, zs: bb[k, xs, zs], put)

    def keep_out(i):
        def put(cc, rows, acc):
            out[rows, pl.ds(pl.multiple_of(keep + i * 2 * W, W), 2 * W)] = acc

        def rhs(xs, zs):
            return jnp.concatenate([bb[2 * i, xs, zs], bb[2 * i + 1, xs, zs]], axis=1)

        multiply(zl, rhs, put)

    def keep_last():
        def put(cc, rows, acc):
            out[rows, pl.ds(pl.multiple_of(keep + (NC - 1) * W, W), W)] = acc

        multiply(zl, lambda xs, zs: bb[NC - 1, xs, zs], put)

    def serve_x(k):
        @pl.when(k + 2 < NC)
        def _():
            fwd_x(k + 2)

        @pl.when(k + 5 < NC)
        def _():
            own_x(k + 5)

        @pl.when(k + 4 < NC)
        def _():
            part_x(k + 4)

    @pl.loop(0, 5)
    def _(k):
        far_x(k)
        give_out(k)

        @pl.when(k == 1)
        def _():
            fwd_y(2)

        @pl.when(k >= 2)
        def _():
            serve_x(k)

        @pl.when(k == 3)
        def _():
            fwd_y(3)

    far_y(2)
    far_y(3)
    scale(2)
    scale(3)

    @pl.loop(5, NC)
    def _(k):
        far_x(k)
        give_out(k)

        @pl.loop(jnp.where(k == 5, 0, k - 4), jnp.minimum(k - 3, 4))
        def _(i):
            keep_out(i)

        serve_x(k)

    keep_last()

    @pl.loop(0, NC)
    def _(k):
        swap(k).wait_send()
        for copy in x_copies(k) + f_copies(k):
            copy.wait_send()
        for cc in range(2):
            c_copy(k, cc).wait()


def on_device(hidden_act, out_grad, other_sq):
    dma = pltpu.SemaphoreType.DMA
    f32, bf16 = jnp.float32, jnp.bfloat16
    anywhere = pl.BlockSpec(memory_space=pltpu.HBM)
    return pl.pallas_call(
        kernel,
        out_shape=pltpu.VMEM((D // 8, COLS), f32),
        in_specs=[anywhere, anywhere, pl.BlockSpec(memory_space=pltpu.SMEM)],
        out_specs=pl.BlockSpec(memory_space=pltpu.VMEM),
        scratch_shapes=[
            pltpu.VMEM((TOK, COLS), bf16),
            pltpu.VMEM((NC, 4, 2, TOK, W), bf16),
            pltpu.VMEM((4, 4, 2 * FEAT, TOK), bf16),
            pltpu.VMEM((2, SUB, TOK), bf16),
            pltpu.VMEM((FEAT, TOK), bf16),
            pltpu.VMEM((2, 2, PACK, W), f32),
            pltpu.VMEM((2, PACK, W), f32),
            pltpu.VMEM((2, PACK, W), f32),
            pltpu.VMEM((3, 2, ROWS, W), f32),
            pltpu.VMEM((2, ROWS, W), f32),
            pltpu.VMEM((2, ROWS, W), f32),
            pltpu.VMEM((4, 8, W), f32),
            pltpu.VMEM((3, 8, W), f32),
            pltpu.VMEM((8, W), f32),
            pltpu.VMEM((8, W), f32),
            pltpu.VMEM((3, 8, W), f32),
            pltpu.VMEM((8, 1, TOK), f32),
            pltpu.VMEM((NC, 2 * FEAT, W), f32),
            dma((2,)), dma((NC,)), dma((2,)), dma((2,)), dma((2,)), dma((2,)), dma((NC,)), dma((NC,)),
            dma((6, NC)), dma((6, NC)), dma((6,)), dma((6,)),
            dma((6, 4)), dma((6, 4)), dma((4, 4)), dma((4, 4)),
            dma((2,)), dma((3,)), dma((3,)), dma((2,)),
            dma((3,)), dma((3,)), dma((4,)), dma((3,)), dma((3,)),
            dma((2, NC)), dma((2, NC)),
        ],
        compiler_params=pltpu.CompilerParams(
            collective_id=0, has_side_effects=True, vmem_limit_bytes=VMEM_LIMIT
        ),
    )(hidden_act, out_grad.T, other_sq)


def solution(mesh):
    torus = Mesh(mesh.devices.reshape(4, 2, 4, 2, 2), AXES)
    dp, tensor = ("x", "zl"), ("y", "zh", "c")
    return jax.shard_map(
        on_device,
        mesh=torus,
        in_specs=(P(dp, tensor), P(dp, tensor), P(dp)),
        out_specs=P(dp, tensor),
        check_vma=False,
    )
```

```python
import functools
import math

import jax
import jax.numpy as jnp
from jax import lax
from jax.experimental import pallas as pl
from jax.experimental.pallas import tpu as pltpu
from jax.sharding import Mesh
from jax.sharding import PartitionSpec as P

D = 4608
FF = 36864
L = 352
TOK = 2 * L
COLS = 2304
HALF = COLS // 2
FEAT = 288
SUB = FEAT // 2
W = 128
VMEM_LIMIT = 61_400_000
NC = HALF // W
AXES = ("x", "zl", "y", "zh", "c")
MESH = pl.DeviceIdType.MESH
BOUND = math.sqrt(L * FF * D / 80.0)
NT = (((1,), (1,)), ((), ()))
PACK = 672
ROWS = PACK // 4


def kernel(
    hid_hbm, gt_hbm, other_ref, out,
    hid, bb, at, tb, gv, gh, rc, rd, ry, r2, rz, tl, ty, tc, tz, tx, sv, cs,
    ld_s, lb_s, t_s, t_r, u_s, u_r, sw_s, sw_r, x_s, x_r, az_s, az_r, ay_s, ay_r, ac_s, ac_r,
    g1_s, g2_s, g2_r, g3_s, t1_s, t1_r, t2_s, t4_s, t4_r, c_s, c_r,
):
    x, zl, y, zh, c = (lax.axis_index(a) for a in AXES)
    z = zh * 2 + zl
    xr, xl, xo = (x + 1) % 4, (x + 3) % 4, (x + 2) % 4
    yr, yl, yo = (y + 1) % 4, (y + 3) % 4, (y + 2) % 4

    def dev(nx=None, nz=None, ny=None, nc=None):
        nz = z if nz is None else nz
        return (
            x if nx is None else nx,
            nz % 2,
            y if ny is None else ny,
            nz // 2,
            c if nc is None else nc,
        )

    zpair = zh * 2 + (1 - zl)

    def send(src, dst, ss, rs, to):
        return pltpu.make_async_remote_copy(
            src_ref=src, dst_ref=dst, send_sem=ss, recv_sem=rs,
            device_id=to, device_id_type=MESH,
        )

    keep = zl * HALF
    give = (1 - zl) * HALF

    load_hid = pltpu.make_async_copy(hid_hbm, hid, ld_s.at[0])
    load_g = pltpu.make_async_copy(gt_hbm, gv, ld_s.at[1])
    load_hid.start()

    def load_own(k):
        col = pl.multiple_of(keep + k * W, W)
        return pltpu.make_async_copy(
            hid_hbm.at[:, pl.ds(col, W)], bb.at[k, x, zl], lb_s.at[k]
        )

    load_g.start()

    @pl.loop(0, NC)
    def _(k):
        load_own(k).start()

    def rows_of(j):
        return pl.ds(pl.multiple_of(j * SUB, 16), SUB)

    def t_copy(r):
        return send(
            gt_hbm.at[pl.ds(r * SUB, SUB)], tb.at[y % 2], t_s.at[r], t_r.at[y % 2],
            dev(ny=2 * c + r, nc=y // 2),
        )

    def t_here(r):
        return pltpu.make_async_copy(
            gt_hbm.at[pl.ds(r * SUB, SUB)], tb.at[y % 2], t_r.at[y % 2]
        )

    def u_copy(i):
        return send(
            tb.at[i], at.at[x, z, rows_of(y)], u_s.at[i], u_r.at[x % 2],
            dev(nx=2 * c + i, nc=x // 2),
        )

    bar = pltpu.get_barrier_semaphore()
    partners = [dev(nx=v) for v in (xr, xl, xo)]
    partners += [dev(ny=v) for v in (yr, yl, yo)]
    partners += [dev(nz=(z + d) % 4) for d in (1, 2, 3)]
    partners += [dev(nc=1 - c)]
    for to in partners:
        pl.semaphore_signal(bar, inc=1, device_id=to, device_id_type=MESH)

    count = len(partners)
    for i in range(2):
        for away, to in (
            (2 * c + i != y, dev(ny=2 * c + i, nc=y // 2)),
            (2 * c + i != x, dev(nx=2 * c + i, nc=x // 2)),
        ):
            count = count + away.astype(jnp.int32)

            @pl.when(away)
            def _():
                pl.semaphore_signal(bar, inc=1, device_id=to, device_id_type=MESH)

    pl.semaphore_wait(bar, count)

    for r in range(2):

        @pl.when(2 * c + r != y)
        def _():
            t_copy(r).start()

        @pl.when(2 * c + r == y)
        def _():
            t_here(r).start()

    def swap(k):
        col = pl.multiple_of(give + k * W, W)
        return send(
            hid.at[:, pl.ds(col, W)], bb.at[k, x, zl], sw_s.at[k], sw_r.at[k],
            dev(nz=zpair),
        )

    def x_copies(k):
        own, swapped = bb.at[k, x, zl], bb.at[k, x, 1 - zl]
        return (
            send(own, own, x_s.at[0, k], x_r.at[0, k], dev(nx=xr)),
            send(own, own, x_s.at[1, k], x_r.at[1, k], dev(nx=xl)),
            send(swapped, swapped, x_s.at[2, k], x_r.at[2, k], dev(nx=xr)),
            send(swapped, swapped, x_s.at[3, k], x_r.at[3, k], dev(nx=xl)),
        )

    def f_copies(k):
        a, b = bb.at[k, xl, 0], bb.at[k, xr, 1]
        return (
            send(a, a, x_s.at[4, k], x_r.at[4, k], dev(nx=xr)),
            send(b, b, x_s.at[5, k], x_r.at[5, k], dev(nx=xl)),
        )

    def own_x(k):
        load_own(k).wait()
        for copy in x_copies(k)[:2]:
            copy.start()

    def part_x(k):
        swap(k).wait_recv()
        for copy in x_copies(k)[2:]:
            copy.start()

    def fwd_x(k):
        for copy in x_copies(k):
            copy.wait_recv()
        for copy in f_copies(k):
            copy.start()

    def far_x(k):
        for copy in f_copies(k):
            copy.wait_recv()

    load_hid.wait()
    swap(0).start()
    swap(1).start()
    own_x(0)
    own_x(1)

    def pack(e, kind, gram):
        gh[e, kind, 0:352, :] = gram[:, 0:128]
        gh[e, kind, 352:576, :] = gram[128:352, 128:256]
        gh[e, kind, 576:672, :] = jnp.zeros((96, W), jnp.float32)
        gh[e, kind, 576:672, 0:96] = gram[256:352, 256:352]

    @pl.loop(0, 2)
    def _(e):
        rows = pl.ds(pl.multiple_of(e * L, 32), L)
        h = hid[rows, :]
        pack(e, 0, lax.dot_general(h, h, NT, preferred_element_type=jnp.float32))

    load_g.wait()
    turned = jnp.transpose(gv[...])
    for e in range(2):
        g = turned[e * L : (e + 1) * L]
        pack(e, 1, lax.dot_general(g, g, NT, preferred_element_type=jnp.float32))

    g1 = send(gh.at[1 - c], rc, g1_s.at[0], g1_s.at[1], dev(nc=1 - c))
    g1.start()

    zr, zb = (z + 1) % 4, (z + 3) % 4

    def piece(i, zz, yy):
        return at.at[2 * c + i, zz, rows_of(yy)]

    def z_copies(i):
        b = piece(i, z, y)
        return (
            send(b, b, az_s.at[i], az_r.at[i], dev(nz=zr)),
            send(b, b, az_s.at[2 + i], az_r.at[2 + i], dev(nz=zb)),
        )

    def zf_copies():
        a, b = piece(0, zb, y), piece(1, zr, y)
        return (
            send(a, a, az_s.at[4], az_r.at[4], dev(nz=zr)),
            send(b, b, az_s.at[5], az_r.at[5], dev(nz=zb)),
        )

    middle = zl != zh
    inner = z // 2 * 2 + (1 - zl)
    outer = (z + 2 * zl + 3) % 4
    across = (z + 2) % 4

    def block(q):
        there = (z, inner, outer, across)[q]
        return jnp.where(middle, there, (outer, across, z, inner)[q])

    def y_copies(q, i):
        b = piece(i, block(q), y)
        return (
            send(b, b, ay_s.at[i, q], ay_r.at[i, q], dev(ny=yr)),
            send(b, b, ay_s.at[2 + i, q], ay_r.at[2 + i, q], dev(ny=yl)),
        )

    def yf_copies(q):
        a, b = piece(0, block(q), yl), piece(1, block(q), yr)
        return (
            send(a, a, ay_s.at[4, q], ay_r.at[4, q], dev(ny=yr)),
            send(b, b, ay_s.at[5, q], ay_r.at[5, q], dev(ny=yl)),
        )

    def core_copy(q, j):
        b = at.at[pl.ds(2 * c, 2), block(q), rows_of((y, yl, yr, yo)[j])]
        return send(b, b, ac_s.at[j, q], ac_r.at[j, q], dev(nc=1 - c))

    def own_y(q):
        for i in range(2):
            for copy in y_copies(q, i):
                copy.start()
        core_copy(q, 0).start()

    def fwd_y(q):
        y_copies(q, 0)[0].wait_recv()
        yf_copies(q)[0].start()
        y_copies(q, 1)[1].wait_recv()
        yf_copies(q)[1].start()
        y_copies(q, 1)[0].wait_recv()
        core_copy(q, 1).start()
        y_copies(q, 0)[1].wait_recv()
        core_copy(q, 2).start()

    def far_y(q):
        for copy in yf_copies(q):
            copy.wait_recv()
        core_copy(q, 3).start()

    def settle(q):
        for copy in y_copies(q, 0) + y_copies(q, 1) + yf_copies(q):
            copy.wait_send()
        for j in range(4):
            core_copy(q, j).wait()

    def scale(q):
        settle(q)

        @pl.loop(0, 8)
        def _(i):
            xs = i // 2
            rows = pl.ds(pl.multiple_of(i % 2 * FEAT, 32), FEAT)
            s = sv[xs * 2 + block(q) % 2]
            b = at[xs, block(q), rows].astype(jnp.float32)
            at[xs, block(q), rows] = (b * s).astype(jnp.bfloat16)

    def g2(d):
        to = (y + d) % 4
        rows = pl.ds(pl.multiple_of(to * ROWS, 8), ROWS)
        return send(
            rd.at[:, rows, :], ry.at[d - 1], g2_s.at[d - 1], g2_r.at[d - 1], dev(ny=to)
        )

    swap(2).start()
    swap(3).start()
    for i in range(2):
        pltpu.make_async_copy(gt_hbm.at[pl.ds(0, SUB)], tb.at[i], t_r.at[i]).wait()

    for i in range(2):
        far_plane = 2 * c + i != x

        @pl.when(far_plane)
        def _():
            u_copy(i).start()

        @pl.when(jnp.logical_not(far_plane))
        def _():
            at[x, z, rows_of(y)] = tb[i]

    part_x(0)
    g1.wait()
    rd[...] = gh[c] + rc[...]
    for d in (2, 1, 3):
        g2(d).start()
    part_x(1)
    own_x(2)

    for i in range(2):

        @pl.when(2 * c + i != x)
        def _():
            send(
                tb.at[i], at.at[2 * c + i, z, rows_of(y)], u_s.at[i], u_r.at[i],
                dev(nx=2 * c + i, nc=x // 2),
            ).wait_recv()

        for copy in z_copies(i):
            copy.start()

        @pl.when(middle)
        def _():
            for copy in y_copies(0, i):
                copy.start()

    @pl.when(middle)
    def _():
        core_copy(0, 0).start()

    own_x(3)
    part_x(2)

    for d in (2, 1, 3):
        g2(d).wait()
    mine = pl.ds(pl.multiple_of(y * ROWS, 8), ROWS)
    r2[...] = rd[:, mine, :] + ry[0] + ry[1] + ry[2]
    g3 = send(r2, rz, g3_s.at[0], g3_s.at[1], dev(nz=across))
    g3.start()

    z_copies(0)[0].wait_recv()
    zf_copies()[0].start()
    z_copies(0)[1].wait_recv()
    z_copies(1)[1].wait_recv()
    zf_copies()[1].start()
    z_copies(1)[0].wait_recv()
    swap(4).start()

    @pl.when(jnp.logical_not(middle))
    def _():
        own_y(0)

    @pl.when(middle)
    def _():
        own_y(1)

    fwd_x(0)
    part_x(3)
    own_x(4)
    fwd_x(1)
    g3.wait()
    total = r2[...] + rz[...]
    at_row = lax.broadcasted_iota(jnp.int32, (ROWS, W), 0) + y * ROWS
    at_lane = lax.broadcasted_iota(jnp.int32, (ROWS, W), 1)
    tile_of = (at_row >= 352).astype(jnp.int32) + (at_row >= 576).astype(jnp.int32)
    over = at_row - jnp.where(tile_of == 0, 0, jnp.where(tile_of == 1, 352, 576)) - at_lane
    weight = jnp.where(over > 0, 2.0, jnp.where(over == 0, 1.0, 0.0))
    part = jnp.sum(total[0] * total[1] * weight)
    lane = lax.broadcasted_iota(jnp.int32, (8, W), 1)
    example = (x * 2 + zl) * 2 + c
    other = jnp.where(c == 0, other_ref[0], other_ref[1])
    tile = jnp.where(lane == example * 4 + y, part, 0.0)
    tl[0] = tile + jnp.where((lane == 64 + example) & (y == 0), other, 0.0)

    def t1(d):
        return send(
            tl.at[0], ty.at[d - 1], t1_s.at[d - 1], t1_r.at[d - 1], dev(ny=(y + d) % 4)
        )

    for d in (2, 1, 3):
        t1(d).start()

    for copy in zf_copies():
        copy.wait_recv()

    @pl.when(jnp.logical_not(middle))
    def _():
        own_y(1)

    swap(5).start()
    fwd_y(0)

    for d in (2, 1, 3):
        t1(d).wait()
    tl[1] = tl[0] + ty[0] + ty[1] + ty[2]
    t2 = send(tl.at[1], tc, t2_s.at[0], t2_s.at[1], dev(nc=1 - c))
    t2.start()
    t2.wait()
    tl[2] = tl[1] + tc[...]
    t3 = send(tl.at[2], tz, t2_s.at[2], t2_s.at[3], dev(nz=zpair))
    t3.start()
    t3.wait()
    tl[3] = tl[2] + tz[...]

    def t4(d):
        return send(
            tl.at[3], tx.at[d - 1], t4_s.at[d - 1], t4_r.at[d - 1], dev(nx=(x + d) % 4)
        )

    for d in (2, 1, 3):
        t4(d).start()

    fwd_x(2)
    part_x(4)
    own_x(5)
    swap(6).start()
    fwd_y(1)
    own_y(2)
    part_x(5)
    own_x(6)
    swap(7).start()
    swap(8).start()
    far_y(0)
    own_y(3)

    for d in (2, 1, 3):
        t4(d).wait()
    full = (tl[3] + tx[0] + tx[1] + tx[2])[0:1]
    row = lax.broadcasted_iota(jnp.int32, (1, W), 1)
    token = lax.broadcasted_iota(jnp.int32, (1, TOK), 1)
    for g in range(8):
        pair = []
        for e in (2 * g, 2 * g + 1):
            layer = jnp.sum(
                jnp.where((row >= 4 * e) & (row < 4 * e + 4), full, 0.0), axis=1, keepdims=True
            )
            rest = jnp.sum(jnp.where(row == 64 + e, full, 0.0), axis=1, keepdims=True)
            pair.append(jnp.minimum(1.0, BOUND / jnp.sqrt(rest + layer)))
        sv[g] = jnp.where(token < L, pair[0], pair[1])

    for i in range(2):

        @pl.when(2 * c + i != y)
        def _():
            t_copy(i).wait_send()

        @pl.when(2 * c + i != x)
        def _():
            u_copy(i).wait_send()

    for copy in z_copies(0) + z_copies(1) + zf_copies():
        copy.wait_send()
    far_y(1)
    fwd_x(3)
    scale(0)
    scale(1)

    def multiply(high, rhs, put):
        @pl.loop(0, 2)
        def _(cc):
            rows = pl.ds(pl.multiple_of(cc * FEAT, 32), FEAT)
            acc = None
            for xs in range(4):
                for zs in range(2):
                    p = jnp.dot(
                        at[xs, high * 2 + zs, rows], rhs(xs, zs),
                        preferred_element_type=jnp.float32,
                    )
                    acc = p if acc is None else acc + p
            put(cc, rows, acc)

    def c_copy(k, cc):
        rows = pl.ds(pl.multiple_of(cc * FEAT, 32), FEAT)
        cols = pl.ds(pl.multiple_of(keep + k * W, W), W)
        return send(
            cs.at[k, rows], out.at[rows, cols], c_s.at[cc, k], c_r.at[cc, k],
            dev(nz=zpair),
        )

    def give_out(k):
        def put(cc, rows, acc):
            cs[k, rows, :] = acc
            c_copy(k, cc).start()

        multiply(1 - zl, lambda xs, zs: bb[k, xs, zs], put)

    def keep_out(i):
        def put(cc, rows, acc):
            out[rows, pl.ds(pl.multiple_of(keep + i * 2 * W, W), 2 * W)] = acc

        def rhs(xs, zs):
            return jnp.concatenate([bb[2 * i, xs, zs], bb[2 * i + 1, xs, zs]], axis=1)

        multiply(zl, rhs, put)

    def keep_last():
        def put(cc, rows, acc):
            out[rows, pl.ds(pl.multiple_of(keep + (NC - 1) * W, W), W)] = acc

        multiply(zl, lambda xs, zs: bb[NC - 1, xs, zs], put)

    def serve_x(k):
        @pl.when(k < 6)
        def _():
            fwd_x(k + 2)

        @pl.when(k == 2)
        def _():
            own_x(7)
            part_x(6)

        @pl.when(k == 3)
        def _():
            part_x(7)

        @pl.when(k == 4)
        def _():
            own_x(8)

        @pl.when(k == 5)
        def _():
            part_x(8)

        @pl.when(k == 7)
        def _():
            fwd_x(8)

    @pl.loop(0, 5)
    def _(k):
        far_x(k)
        give_out(k)

        @pl.when(k == 1)
        def _():
            fwd_y(2)

        @pl.when(k >= 2)
        def _():
            serve_x(k)

        @pl.when(k == 3)
        def _():
            fwd_y(3)

    far_y(2)
    far_y(3)
    scale(2)
    scale(3)

    @pl.loop(5, NC)
    def _(k):
        far_x(k)
        give_out(k)

        @pl.loop(jnp.where(k == 5, 0, k - 4), jnp.minimum(k - 3, 4))
        def _(i):
            keep_out(i)

        serve_x(k)

    keep_last()

    @pl.loop(0, NC)
    def _(k):
        swap(k).wait_send()
        for copy in x_copies(k) + f_copies(k):
            copy.wait_send()
        for cc in range(2):
            c_copy(k, cc).wait()


def on_device(hidden_act, out_grad, other_sq):
    dma = pltpu.SemaphoreType.DMA
    f32, bf16 = jnp.float32, jnp.bfloat16
    anywhere = pl.BlockSpec(memory_space=pltpu.HBM)
    return pl.pallas_call(
        kernel,
        out_shape=pltpu.VMEM((D // 8, COLS), f32),
        in_specs=[anywhere, anywhere, pl.BlockSpec(memory_space=pltpu.SMEM)],
        out_specs=pl.BlockSpec(memory_space=pltpu.VMEM),
        scratch_shapes=[
            pltpu.VMEM((TOK, COLS), bf16),
            pltpu.VMEM((NC, 4, 2, TOK, W), bf16),
            pltpu.VMEM((4, 4, 2 * FEAT, TOK), bf16),
            pltpu.VMEM((2, SUB, TOK), bf16),
            pltpu.VMEM((FEAT, TOK), bf16),
            pltpu.VMEM((2, 2, PACK, W), f32),
            pltpu.VMEM((2, PACK, W), f32),
            pltpu.VMEM((2, PACK, W), f32),
            pltpu.VMEM((3, 2, ROWS, W), f32),
            pltpu.VMEM((2, ROWS, W), f32),
            pltpu.VMEM((2, ROWS, W), f32),
            pltpu.VMEM((4, 8, W), f32),
            pltpu.VMEM((3, 8, W), f32),
            pltpu.VMEM((8, W), f32),
            pltpu.VMEM((8, W), f32),
            pltpu.VMEM((3, 8, W), f32),
            pltpu.VMEM((8, 1, TOK), f32),
            pltpu.VMEM((NC, 2 * FEAT, W), f32),
            dma((2,)), dma((NC,)), dma((2,)), dma((2,)), dma((2,)), dma((2,)), dma((NC,)), dma((NC,)),
            dma((6, NC)), dma((6, NC)), dma((6,)), dma((6,)),
            dma((6, 4)), dma((6, 4)), dma((4, 4)), dma((4, 4)),
            dma((2,)), dma((3,)), dma((3,)), dma((2,)),
            dma((3,)), dma((3,)), dma((4,)), dma((3,)), dma((3,)),
            dma((2, NC)), dma((2, NC)),
        ],
        compiler_params=pltpu.CompilerParams(
            collective_id=0, has_side_effects=True, vmem_limit_bytes=VMEM_LIMIT
        ),
    )(hidden_act, out_grad.T, other_sq)


def solution(mesh):
    torus = Mesh(mesh.devices.reshape(4, 2, 4, 2, 2), AXES)
    dp, tensor = ("x", "zl"), ("y", "zh", "c")
    return jax.shard_map(
        on_device,
        mesh=torus,
        in_specs=(P(dp, tensor), P(dp, tensor), P(dp)),
        out_specs=P(dp, tensor),
        check_vma=False,
    )
```
